32 devices in a mesh: pipe: 8 (over z, y), tensor: 4 (over x, core).
Axes of the slice: x: 2, y: 2, z: 4, core: 2. Of those that a mesh axis runs over, the one named last changes fastest.
Arguments:
- memory: bfloat16 [2, 512, 4096], P(None, 'pipe', 'tensor'), may hold values from -6 to 6
- states: bfloat16 [8, 2, 256, 4096], P('pipe', None, None, 'tensor'), may hold values from -6 to 6
- norm_gain: float32 [8, 4096], P('pipe'), may hold values from 0.25 to 1.75
- w_query: bfloat16 [8, 4096, 4096], P('pipe', None, 'tensor'), may hold values from -0.09375 to 0.09375
- w_keyvalue: bfloat16 [8, 4096, 2, 4096], P('pipe', None, None, 'tensor'), may hold values from -0.09375 to 0.09375
- w_output: bfloat16 [8, 4096, 4096], P('pipe', 'tensor'), may hold values from -0.125 to 0.125
Outputs:
- updated: bfloat16 [8, 2, 256, 4096], P('pipe', None, None, 'tensor')
The draws below stay inside these ranges and needn't reach their ends.
All inputs are finite; a program needn't handle non-finite values.
Results may differ from the reference program's by a relative error of at most 0.006.
Values may be sent and summed in bfloat16 or wider, within the bound.
A program may use at most 128 MiB of HBM per device.

```python
import jax
import jax.numpy as jnp
from jax import lax

D = 4096
HEADS = 64
HEAD_DIM = 64
INNER = 4096
SEQS = 2
ENC_LEN = 512
DEC_LEN = 256
SECTIONS = 8


def with_spikes(entries, stream_key, source, target, parts, factor):
    owner, partner = [(jnp.arange(entries.shape[dim]) // (entries.shape[dim] // parts)).reshape([-1 if axis == dim else 1 for axis in range(entries.ndim)]) for dim in (source, target)]
    chosen = jax.random.permutation(stream_key, parts)[partner]
    strong = (owner == chosen) | (owner == (partner + parts // 2) % parts)
    return jnp.where(strong, factor * entries, entries)


def levels(own_key, extent, shards, low, largest):
    level, own = 1.0, jax.random.fold_in(own_key, 6)
    for dim, parts in shards:
        steps = jnp.exp(jax.random.uniform(jax.random.fold_in(own, dim), (parts,), jnp.float32, low / len(shards), largest / len(shards)))
        level = level * jnp.repeat(steps, extent[dim] // parts).reshape([-1 if axis == dim else 1 for axis in range(len(extent))])
    return level


def scatter_about(rng, extent, scale, reach, split=(), held_as=jnp.bfloat16):
    result = jax.random.normal(rng, extent, jnp.float32) * scale
    if len(split) > 0:
        result = levels(rng, extent, split, -0.22, 0.18) * result
    return jnp.clip(result, min=-reach, max=reach).astype(held_as)


def noise_with(own_key, shape, spread, reach, split, heavy, dtype=jnp.bfloat16):
    values = spread * jax.random.normal(own_key, shape, jnp.float32)
    if split:
        values = values * levels(own_key, shape, split, -0.22, 0.18)
    return jnp.clip(with_spikes(values, jax.random.fold_in(own_key, 3), *heavy), -reach, reach).astype(dtype)


def setup_inputs(seed: int = 0) -> dict:
    key_of = jax.random.split(jax.random.key(seed), 7)
    return {
        "memory": scatter_about(key_of[0], (SEQS, ENC_LEN, D), 1.0, 6.0, ((1, 8), (2, 4))),
        "states": scatter_about(key_of[1], (SECTIONS, SEQS, DEC_LEN, D), 1.0, 6.0, ((0, 8), (3, 4))),
        "norm_gain": jnp.clip(1.0 + 0.15 * jax.random.normal(key_of[2], (SECTIONS, D), jnp.float32), 0.25, 1.75),
        "w_query": scatter_about(key_of[3], (SECTIONS, D, INNER), D ** -0.5, 0.09375, ((0, 8), (2, 4))),
        "w_keyvalue": scatter_about(key_of[4], (SECTIONS, D, 2, INNER), D ** -0.5, 0.09375, ((0, 8), (3, 4))),
        "w_output": noise_with(key_of[5], (SECTIONS, INNER, D), INNER ** -0.5, 0.125, ((0, 8), (1, 4)), (1, 2, 4, 2.0)),
    }


def one_section(memory, section_states, gain, wq, wkv, wo):
    xf = section_states.astype(jnp.float32)
    scale = lax.rsqrt(lax.optimization_barrier(jnp.mean(xf * xf, axis=-1, keepdims=True)) + 1e-06)
    normed = (xf * scale * gain).astype(jnp.bfloat16)
    seqs = normed.shape[0]
    inner = HEADS * HEAD_DIM
    wkv_flat = wkv.reshape(wkv.shape[0], 2 * inner)
    query = jnp.einsum('btd,de->bte', normed.astype(jnp.float32), wq.astype(jnp.float32)).astype(jnp.bfloat16)
    keyvalue = jnp.einsum('bpd,de->bpe', memory.astype(jnp.float32), wkv_flat.astype(jnp.float32)).astype(jnp.bfloat16)
    keys = keyvalue[:, :, :inner].reshape(seqs, ENC_LEN, HEADS, HEAD_DIM)
    values = keyvalue[:, :, inner:].reshape(seqs, ENC_LEN, HEADS, HEAD_DIM)
    qh = query.reshape(seqs, DEC_LEN, HEADS, HEAD_DIM)
    scores = jnp.einsum('bqhd,bkhd->bhqk', qh.astype(jnp.float32), keys.astype(jnp.float32)) / jnp.sqrt(jnp.float32(HEAD_DIM))
    probs = jax.nn.softmax(scores, axis=-1).astype(jnp.bfloat16)
    context = jnp.einsum('bhqk,bkhd->bqhd', probs.astype(jnp.float32), values.astype(jnp.float32)).astype(jnp.bfloat16)
    context = context.reshape(seqs, DEC_LEN, inner)
    branch = jnp.einsum('bte,ed->btd', context.astype(jnp.float32), wo.astype(jnp.float32))
    return (xf + branch).astype(jnp.bfloat16)

def reference(memory, states, norm_gain, w_query, w_keyvalue, w_output):

    def run(packed):
        section_states, gain, wq, wkv, wo = packed
        return one_section(memory, section_states, gain, wq, wkv, wo)
    return lax.map(run, (states, norm_gain, w_query, w_keyvalue, w_output))
```

```python
import functools

import jax
import jax.numpy as jnp
from jax import lax
from jax.experimental import pallas as pl
from jax.experimental.pallas import tpu as pltpu
from jax.sharding import PartitionSpec as P

HEAD_DIM = 64
CORES = 2
LOW = 2
TILE = 256
WIDE = 512
MAX_COPIES = 100
LANES = 128
SUB = 16
CHUNK = 256
SLOTS = 3
MESH = pl.DeviceIdType.MESH
F32 = jnp.float32
BF16 = jnp.bfloat16


def copies_per_sequence(n_pipe, n_tensor):
    xs, highs = n_tensor // CORES, n_pipe // LOW
    return 4 * n_pipe * xs + (xs - 1) * highs


def kernel(
    n_pipe, n_tensor,
    mem_hbm, st_hbm, gain_ref, wq_hbm, wkv_hbm, wo_hbm, out_hbm,
    mem, st, wq, wkv, wo, q, kv, ctx, pd, rd, px, rx, part, staged, squares, done,
    load_sem, stage_sem, send_sem, recv_ici, recv_d2d, st_ici, st_d2d, pd_sem, px_sem, out_sem,
):
    xs, highs = n_tensor // CORES, n_pipe // LOW
    seqs, enc, depth = mem.shape
    rows = st.shape[1]
    pos = enc // n_pipe
    feat = depth // n_tensor
    inner = wq.shape[1]
    pipe = lax.axis_index("pipe")
    tensor = lax.axis_index("tensor")
    hi, lo = pipe // LOW, pipe % LOW
    x, core = tensor // CORES, tensor % CORES
    other_lo, other_core = 1 - lo, 1 - core
    scope = jax.named_scope

    def turn(a, k, n):
        return lax.rem(a + k, n)

    def device(h, l, xx, c):
        return (h * LOW + l, xx * CORES + c)

    x_peers = [device(hi, lo, turn(x, j, xs), core) for j in range(1, xs)]
    hi_peers = [device(turn(hi, k, highs), lo, x, core) for k in range(1, highs)]
    lo_peer = device(hi, other_lo, x, core)
    sibling = device(hi, lo, x, other_core)

    def block(s, h, far, xx, c):
        r = pl.multiple_of((far * highs + h) * pos, pos)
        f = pl.multiple_of((xx * CORES + c) * feat, feat)
        return mem.at[s, pl.ds(r, pos), pl.ds(f, feat)]

    def slot(h, l, xx):
        return (h * LOW + l) * xs + xx

    def st_block(s, xx, c):
        return st.at[s, :, pl.ds(pl.multiple_of((xx * CORES + c) * feat, feat), feat)]

    counter = [0]
    waits = []

    def remote(src, dst, sem, recv, dev):
        return pltpu.make_async_remote_copy(
            src_ref=src, dst_ref=dst, send_sem=send_sem.at[sem], recv_sem=recv,
            device_id=dev, device_id_type=MESH,
        )

    def send(src, dst, recv, dev, like, keep=True):
        sem = counter[0]
        counter[0] += 1
        remote(src, dst, sem, recv, dev).start()
        if keep:
            waits.append((like, sem))
        return sem

    def sent(like, sem):
        remote(like, like, sem, recv_ici.at[0, 0], sibling).wait_send()

    def like_block():
        return block(0, 0, 0, 0, 0)

    def send_own(s, h, xx, dev, recv):
        ref = block(s, h, 0, xx, core)
        send(ref, ref, recv.at[s, slot(h, lo, xx)], dev, like_block)

    def send_low(s, h, xx):
        send(block(s, h, 0, xx, core), block(s, h, 1, xx, core),
             recv_ici.at[s, slot(h, lo, xx)], lo_peer, like_block)

    def send_far(s, h, xx):
        ref = block(s, h, 1, xx, core)
        send(ref, ref, recv_d2d.at[s, slot(h, other_lo, xx)], sibling, like_block)

    def arrived(s, h, l, xx, recv):
        ref = like_block()
        remote(ref, ref, 0, recv.at[s, slot(h, l, xx)], sibling).wait_recv()

    st_sends = [[], []]

    def first_send(s):
        def low():
            send_low(s, hi, x)

        def across():
            for dev in x_peers:
                send_own(s, hi, x, dev, recv_ici)

        def high():
            for dev in hi_peers:
                send_own(s, hi, x, dev, recv_ici)

        def over():
            send_own(s, hi, x, sibling, recv_d2d)

        return low, across, high, over

    def state_sends(s):
        ref = st_block(s, x, core)
        for dev in x_peers:
            st_sends[s].append(send(ref, ref, st_ici.at[s, x], dev, None, False))
        st_sends[s].append(send(ref, ref, st_d2d.at[s, x], sibling, None, False))

    def forward_x(s):
        for j in range(1, xs):
            xx = turn(x, j, xs)
            arrived(s, hi, lo, xx, recv_ici)
            send_low(s, hi, xx)
            for dev in hi_peers:
                send_own(s, hi, xx, dev, recv_ici)
            send_own(s, hi, xx, sibling, recv_d2d)

    high_order = [(k, j) for j in range(xs) for k in range(highs - 1, 0, -1)]
    low_order = [(0, j) for j in range(xs)] + high_order

    def forward_high(s, i):
        k, j = high_order[i]
        h, xx = turn(hi, k, highs), turn(x, j, xs)
        arrived(s, h, lo, xx, recv_ici)
        send_low(s, h, xx)
        send_own(s, h, xx, sibling, recv_d2d)

    def forward_low(s, i):
        k, j = low_order[i]
        h, xx = turn(hi, k, highs), turn(x, j, xs)
        arrived(s, h, other_lo, xx, recv_ici)
        send_far(s, h, xx)

    def forward_states(s):
        for j in range(1, xs):
            xx = turn(x, j, xs)
            ref = st_block(s, xx, core)
            remote(ref, ref, 0, st_ici.at[s, xx], sibling).wait_recv()
            st_sends[s].append(send(ref, ref, st_d2d.at[s, xx], sibling, None, False))

    def finish_states(s):
        for xx in range(xs):
            ref = st_block(s, xx, other_core)
            remote(ref, ref, 0, st_d2d.at[s, xx], sibling).wait_recv()
        for sem in st_sends[s]:
            sent(st_block(s, x, core), sem)

    def finish_memory(s, far):
        for h in range(highs):
            for xx in range(xs):
                arrived(s, h, other_lo if far else lo, xx, recv_d2d)

    def steps(n, body, plan=()):
        plan = dict(plan)
        assert all(t < n for t in plan)

        @pl.loop(0, n)
        def _(i):
            for t, events in plan.items():
                @pl.when(i == t)
                def _(events=events):
                    for fn, *args in events:
                        fn(*args)

            body(i)

    def do(*events):
        for fn, *args in events:
            fn(*args)

    def normalize(s):
        part[s] = st[s, :, pl.ds(pl.multiple_of(tensor * feat, feat), feat)].astype(F32)

        @pl.loop(0, rows // SUB)
        def _(i):
            some = pl.ds(pl.multiple_of(i * SUB, SUB), SUB)
            total = jnp.zeros((SUB, LANES), F32)
            for g in range(depth // LANES):
                cols = slice(g * LANES, (g + 1) * LANES)
                xf = st[s, some, cols].astype(F32)
                total += xf * xf
                st[s, some, cols] = (xf * gain_ref[:, cols]).astype(BF16)
            squares[some, :] = total

        mean = jnp.sum(squares[...], axis=-1, keepdims=True) * (1.0 / depth)
        scale = lax.rsqrt(mean + 1e-06) * (HEAD_DIM ** -0.5)
        squares[...] = jnp.broadcast_to(scale, squares.shape)

    def query(s, plan):
        def body(i):
            cols = pl.ds(pl.multiple_of(i * TILE, TILE), TILE)
            full = jnp.dot(st[s], wq[:, cols], preferred_element_type=F32)
            scale = squares[...]
            q[s, :, cols] = (full * jnp.concatenate([scale] * (TILE // LANES), axis=1)).astype(BF16)

        steps(inner // TILE, body, plan)

    half = highs * pos

    def keyvalue(s, far, plan):
        def body(i):
            cols = pl.ds(pl.multiple_of(i * WIDE, WIDE), WIDE)
            full = jnp.dot(mem[s, far * half:(far + 1) * half], wkv[:, cols], preferred_element_type=F32)
            kv[far * half:(far + 1) * half, cols] = full.astype(BF16)

        steps(2 * inner // WIDE, body, plan)

    PAIRS = 2

    def attention(s, plan):
        lane = lax.broadcasted_iota(jnp.int32, (1, 2 * HEAD_DIM), 1)
        first = lane < HEAD_DIM

        def body(step):
            for u in range(PAIRS):
                i = step * PAIRS + u
                cols = pl.ds(pl.multiple_of(i * 2 * HEAD_DIM, 2 * HEAD_DIM), 2 * HEAD_DIM)
                vcols = pl.ds(pl.multiple_of(inner + i * 2 * HEAD_DIM, 2 * HEAD_DIM), 2 * HEAD_DIM)
                qp, kp, vp = q[s, :, cols], kv[:, cols], kv[:, vcols]
                outs = []
                for mine in (first, jnp.logical_not(first)):
                    qh = jnp.where(mine, qp, jnp.zeros_like(qp))
                    vh = jnp.where(mine, vp, jnp.ones_like(vp))
                    scores = lax.dot_general(
                        qh, kp, (((1,), (1,)), ((), ())), preferred_element_type=F32
                    )
                    top = jnp.max(scores, axis=-1, keepdims=True)
                    probs = jnp.exp(scores - top).astype(BF16)
                    outs.append(jnp.dot(probs, vh, preferred_element_type=F32))
                total = jnp.where(first, outs[0], outs[1])
                sums = pltpu.roll(jnp.where(first, outs[1], outs[0]), HEAD_DIM, 1)
                ctx[:, cols] = (total / sums).astype(BF16)

        steps(inner // (2 * HEAD_DIM * PAIRS), body, plan)

    width = min(WIDE, feat)
    tiles = feat // width

    def product(t, i):
        cols = pl.ds(pl.multiple_of(t * feat + i * width, width), width)
        return jnp.dot(ctx[...], wo[:, cols], preferred_element_type=F32)

    def output(s):
        order = [turn(x, j, xs) for j in range(1, xs)] + [x]

        def over(j, i):
            c = slice(i * width, (i + 1) * width)
            pd[s, j, :, c] = product(order[j] * CORES + other_core, i).astype(BF16)
            send(pd.at[s, j, :, c], rd.at[s, j, :, c], pd_sem.at[s, j, i], sibling,
                 lambda: pd.at[0, 0, :, :width])

        def back(j, i):
            c = slice(i * width, (i + 1) * width)
            remote(pd.at[s, j, :, c], rd.at[s, j, :, c], 0, pd_sem.at[s, j, i], sibling).wait_recv()

        for j in range(xs - 1):
            for i in range(tiles):
                over(j, i)
            for i in range(tiles):
                c = slice(i * width, (i + 1) * width)
                mine = product(order[j] * CORES + core, i)
                back(j, i)
                px[s, j, :, c] = (mine + rd[s, j, :, c].astype(F32)).astype(BF16)
                send(px.at[s, j, :, c], rx.at[s, j, :, c], px_sem.at[s, j, i], x_peers[j],
                     lambda: pd.at[0, 0, :, :width])
        j = xs - 1
        for i in range(tiles):
            over(j, i)
        for i in range(tiles):
            c = slice(i * width, (i + 1) * width)
            part[s, :, c] += product(tensor, i)
        for i in range(tiles):
            c = slice(i * width, (i + 1) * width)
            back(j, i)
            part[s, :, c] += rd[s, j, :, c].astype(F32)

    def out_copy(s, i):
        c = slice(i * width, (i + 1) * width)
        return pltpu.make_async_copy(done.at[s, :, c], out_hbm.at[s, :, c], out_sem.at[s, i])

    def finish(s):
        for i in range(tiles):
            c = slice(i * width, (i + 1) * width)
            total = part[s, :, c]
            for j in range(xs - 1):
                remote(px.at[s, j, :, c], rx.at[s, j, :, c], 0, px_sem.at[s, j, i], sibling).wait_recv()
                total += rx[s, j, :, c].astype(F32)
            done[s, :, c] = total.astype(BF16)
            out_copy(s, i).start()

    groups = 2 * inner // LANES
    size = CHUNK * groups
    chunks = depth // CHUNK
    slots = staged.shape[0]

    def stage(i, slot):
        src = wkv_hbm.at[pl.ds(pl.multiple_of(i * size, size), size), :]
        return pltpu.make_async_copy(src, staged.at[slot], stage_sem.at[slot])

    def spread(plan):
        span = SUB * groups
        a = lax.broadcasted_iota(jnp.int32, (span, span), 0)
        b = lax.broadcasted_iota(jnp.int32, (span, span), 1)
        swap = (b == lax.rem(a, SUB) * groups + a // SUB).astype(F32).astype(BF16)

        def body(i):
            slot = lax.rem(i, slots)
            stage(i, slot).wait()
            for m in range(CHUNK // (2 * SUB)):
                r = m * 2 * span
                both = jnp.concatenate(
                    [staged[slot, r:r + span, :], staged[slot, r + span:r + 2 * span, :]], axis=1
                )
                moved = jnp.dot(swap, both, preferred_element_type=F32).astype(BF16)
                d = pl.multiple_of(i * CHUNK + m * 2 * SUB, 2 * SUB)
                for g in range(groups):
                    col = (g % 2) * inner + (g // 2) * LANES
                    piece = moved[g * SUB:(g + 1) * SUB]
                    wkv[pl.ds(d, SUB), col:col + LANES] = piece[:, :LANES]
                    wkv[pl.ds(d + SUB, SUB), col:col + LANES] = piece[:, LANES:]

            @pl.when(i + slots < chunks)
            def _():
                stage(i + slots, slot).start()

        steps(chunks, body, plan)

    loads = [
        pltpu.make_async_copy(mem_hbm.at[0], block(0, hi, 0, x, core), load_sem.at[0]),
        pltpu.make_async_copy(st_hbm.at[0], st_block(0, x, core), load_sem.at[1]),
        pltpu.make_async_copy(mem_hbm.at[1], block(1, hi, 0, x, core), load_sem.at[2]),
        pltpu.make_async_copy(st_hbm.at[1], st_block(1, x, core), load_sem.at[3]),
    ]
    weights = [
        pltpu.make_async_copy(wq_hbm, wq, load_sem.at[4]),
        pltpu.make_async_copy(wo_hbm, wo, load_sem.at[5]),
    ]
    for copy in loads:
        copy.start()
    barrier = pltpu.get_barrier_semaphore()
    peers = x_peers + hi_peers + [lo_peer, sibling]
    for peer in peers:
        pl.semaphore_signal(barrier, inc=1, device_id=peer, device_id_type=MESH)
    for i in range(slots):
        stage(i, i).start()
    for copy in weights:
        copy.start()
    with scope("barrier"):
        pl.semaphore_wait(barrier, len(peers))
    with scope("load0"):
        loads[0].wait()
    low, across, high, over = first_send(0)
    across(), low(), high(), over()
    with scope("load1"):
        loads[1].wait()
    state_sends(0)
    loads[2].wait()
    loads[3].wait()
    low1, across1, high1, over1 = first_send(1)

    def second_start():
        high1()
        across1()
        over1()
        state_sends(1)

    def fx(s): forward_x(s)
    def fh(s, i): forward_high(s, i)
    def fl(s, i): forward_low(s, i)

    with scope("spread"):
        spread({
            8: [(fx, 0), (second_start,)],
            9: [(fl, 0, 0)],
            10: [(fh, 0, 0)],
            12: [(fh, 0, 1)],
            14: [(fl, 0, 1)],
        })
    with scope("fh02"):
        fh(0, 2)
    with scope("fl02"):
        fl(0, 2)
    with scope("fh03"):
        fh(0, 3)
    low1()
    with scope("fl03"):
        fl(0, 3)
    with scope("fst0"):
        forward_states(0)
    with scope("finst0"):
        finish_states(0)
    with scope("norm0"):
        normalize(0)
    with scope("wq"):
        weights[0].wait()
    with scope("query0"):
        query(0, {0: [(fh, 0, 4)], 1: [(fl, 0, 4)], 2: [(fh, 0, 5)], 3: [(fl, 0, 5)]})
    with scope("finmem00"):
        finish_memory(0, 0)
    with scope("kv00"):
        keyvalue(0, 0, {0: [(fx, 1)], 1: [(fl, 0, 6)], 2: [(fh, 1, 0)], 3: [(fl, 0, 7)]})
    with scope("finmem01"):
        finish_memory(0, 1)
    with scope("kv01"):
        keyvalue(0, 1, {0: [(fh, 1, 1)], 1: [(fl, 1, 0)], 2: [(fh, 1, 2)], 3: [(fl, 1, 1)]})
    with scope("att0"):
        attention(0, {0: [(fh, 1, 3)], 1: [(fl, 1, 2)], 2: [(fh, 1, 4), (forward_states, 1)], 3: [(fl, 1, 3)]})
    with scope("fh15"):
        fh(1, 5)
    with scope("finst1"):
        finish_states(1)
    with scope("norm1"):
        normalize(1)
    with scope("query1"):
        query(1, {1: [(fl, 1, 4)], 3: [(fl, 1, 5)]})
    weights[1].wait()
    with scope("output0"):
        output(0)
    with scope("finmem10"):
        finish_memory(1, 0)
    with scope("kv10"):
        keyvalue(1, 0, {1: [(fl, 1, 6)], 3: [(fl, 1, 7)]})
    with scope("finmem11"):
        finish_memory(1, 1)
    with scope("kv11"):
        keyvalue(1, 1, {})
    with scope("finish0"):
        finish(0)
    with scope("att1"):
        attention(1, {})
    with scope("output1"):
        output(1)
    with scope("finish1"):
        finish(1)
    with scope("end"):
        for like, sem in waits:
            sent(like(), sem)
        for s in range(seqs):
            for i in range(tiles):
                out_copy(s, i).wait()


def fused(n_pipe, n_tensor, memory, states, norm_gain, w_query, w_keyvalue, w_output):
    seqs, pos, feat = memory.shape
    rows = states.shape[2]
    depth, inner = feat * n_tensor, w_query.shape[2]
    enc = pos * n_pipe
    xs, highs = n_tensor // CORES, n_pipe // LOW
    groups = 2 * inner // LANES
    weight_kv = w_keyvalue[0].reshape(depth, 2, inner // LANES, LANES)
    weight_kv = weight_kv.transpose(0, 2, 1, 3).reshape(depth * groups, LANES)
    blocks = n_pipe * xs
    tiles = feat // min(WIDE, feat)
    per_seq = ((xs - 1) + (highs - 1) + 2 + (xs - 1) * (highs + 1) + 2 * (highs - 1) * xs
               + highs * xs + 2 * xs + 2 * xs * tiles)
    any_space = pl.BlockSpec(memory_space=pl.ANY)
    in_vmem = pl.BlockSpec(memory_space=pltpu.VMEM)
    dma = pltpu.SemaphoreType.DMA
    out = pl.pallas_call(
        functools.partial(kernel, n_pipe, n_tensor),
        out_shape=jax.ShapeDtypeStruct((seqs, rows, feat), BF16),
        in_specs=[any_space, any_space, in_vmem, any_space, any_space, any_space],
        out_specs=any_space,
        scratch_shapes=[
            pltpu.VMEM((seqs, enc, depth), BF16),
            pltpu.VMEM((seqs, rows, depth), BF16),
            pltpu.VMEM((depth, inner), BF16),
            pltpu.VMEM((depth, 2 * inner), BF16),
            pltpu.VMEM((inner, depth), BF16),
            pltpu.VMEM((seqs, rows, inner), BF16),
            pltpu.VMEM((enc, 2 * inner), BF16),
            pltpu.VMEM((rows, inner), BF16),
            pltpu.VMEM((seqs, xs, rows, feat), BF16),
            pltpu.VMEM((seqs, xs, rows, feat), BF16),
            pltpu.VMEM((seqs, xs - 1, rows, feat), BF16),
            pltpu.VMEM((seqs, xs - 1, rows, feat), BF16),
            pltpu.VMEM((seqs, rows, feat), F32),
            pltpu.VMEM((SLOTS, CHUNK * groups, LANES), BF16),
            pltpu.VMEM((rows, LANES), F32),
            pltpu.VMEM((seqs, rows, feat), BF16),
            dma((6,)),
            dma((SLOTS,)),
            dma((seqs * per_seq,)),
            dma((seqs, blocks)),
            dma((seqs, blocks)),
            dma((seqs, xs)),
            dma((seqs, xs)),
            dma((seqs, xs, tiles)),
            dma((seqs, xs - 1, tiles)),
            dma((seqs, tiles)),
        ],
        compiler_params=pltpu.CompilerParams(
            collective_id=0, has_side_effects=True, vmem_limit_bytes=66_000_000
        ),
    )(memory, states[0], norm_gain, w_query[0], weight_kv, w_output[0])
    return out[None]


def per_device(memory, states, norm_gain, w_query, w_keyvalue, w_output):
    whole_states = lax.all_gather(states[0], "tensor", axis=2, tiled=True)
    xf = whole_states.astype(jnp.float32)
    scale = lax.rsqrt(jnp.mean(xf * xf, axis=-1, keepdims=True) + 1e-06)
    normed = (xf * scale * norm_gain[0]).astype(jnp.bfloat16)
    weight_q = w_query[0]
    local_inner = weight_q.shape[1]
    weight_kv = w_keyvalue[0].reshape(w_keyvalue.shape[1], 2 * local_inner)
    weight_o = w_output[0]
    seqs = normed.shape[0]
    dec_rows = normed.shape[1]
    local_heads = local_inner // HEAD_DIM
    query = jnp.einsum("btd,de->bte", normed, weight_q, preferred_element_type=jnp.float32).astype(
        jnp.bfloat16
    )
    gathered = lax.all_gather(memory, "pipe", axis=1, tiled=True)
    gathered = lax.all_gather(gathered, "tensor", axis=2, tiled=True)
    keyvalue = jnp.einsum(
        "bpd,de->bpe", gathered, weight_kv, preferred_element_type=jnp.float32
    ).astype(jnp.bfloat16)
    enc_rows = keyvalue.shape[1]
    keys = keyvalue[:, :, :local_inner].reshape(seqs, enc_rows, local_heads, HEAD_DIM)
    values = keyvalue[:, :, local_inner:].reshape(seqs, enc_rows, local_heads, HEAD_DIM)
    heads_q = query.reshape(seqs, dec_rows, local_heads, HEAD_DIM)
    scores = jnp.einsum(
        "bqhd,bkhd->bhqk", heads_q, keys, preferred_element_type=jnp.float32
    ) / jnp.sqrt(jnp.float32(HEAD_DIM))
    probs = jax.nn.softmax(scores, axis=-1).astype(jnp.bfloat16)
    context = jnp.einsum(
        "bhqk,bkhd->bqhd", probs, values, preferred_element_type=jnp.float32
    ).astype(jnp.bfloat16)
    context = context.reshape(seqs, dec_rows, local_inner)
    partial_terms = jnp.einsum("bte,ed->btd", context, weight_o, preferred_element_type=jnp.float32)
    branch = lax.psum_scatter(partial_terms, "tensor", scatter_dimension=2, tiled=True)
    result = (states[0].astype(jnp.float32) + branch).astype(jnp.bfloat16)
    return result[None]


def solution(mesh):
    in_specs = (
        P(None, "pipe", "tensor"),
        P("pipe", None, None, "tensor"),
        P("pipe", None),
        P("pipe", None, "tensor"),
        P("pipe", None, None, "tensor"),
        P("pipe", "tensor", None),
    )
    out_specs = P("pipe", None, None, "tensor")
    n_pipe, n_tensor = mesh.shape["pipe"], mesh.shape["tensor"]
    even = n_pipe % LOW == 0 and n_tensor % CORES == 0 and n_pipe > LOW and n_tensor > CORES
    body = per_device
    if even and copies_per_sequence(n_pipe, n_tensor) <= MAX_COPIES:
        body = functools.partial(fused, n_pipe, n_tensor)
    return jax.shard_map(
        body, mesh=mesh, in_specs=in_specs, out_specs=out_specs, check_vma=False
    )
```

```python
import functools

import jax
import jax.numpy as jnp
from jax import lax
from jax.experimental import pallas as pl
from jax.experimental.pallas import tpu as pltpu
from jax.sharding import PartitionSpec as P

HEAD_DIM = 64
CORES = 2
LOW = 2
TILE = 256
WIDE = 512
MAX_COPIES = 100
LANES = 128
SUB = 16
CHUNK = 256
SLOTS = 3
PAIRS = 4
MESH = pl.DeviceIdType.MESH
F32 = jnp.float32
BF16 = jnp.bfloat16


def copies_per_sequence(n_pipe, n_tensor):
    xs, highs = n_tensor // CORES, n_pipe // LOW
    return 4 * n_pipe * xs + (xs - 1) * highs


def kernel(
    n_pipe, n_tensor,
    mem_hbm, st_hbm, gain_ref, wq_hbm, wkv_hbm, wo_hbm, out_hbm,
    mem, st, wq, wkv, wo, q, kv, ctx, pd, rd, px, rx, part, staged, squares,
    load_sem, stage_sem, send_sem, recv_ici, recv_d2d, st_ici, st_d2d, pd_sem, px_sem, out_sem,
):
    xs, highs = n_tensor // CORES, n_pipe // LOW
    seqs, enc, depth = mem.shape
    rows = st.shape[1]
    pos = enc // n_pipe
    feat = depth // n_tensor
    inner = wq.shape[1]
    pipe = lax.axis_index("pipe")
    tensor = lax.axis_index("tensor")
    hi, lo = pipe // LOW, pipe % LOW
    x, core = tensor // CORES, tensor % CORES
    other_lo, other_core = 1 - lo, 1 - core
    scope = jax.named_scope

    def turn(a, k, n):
        return lax.rem(a + k, n)

    def device(h, l, xx, c):
        return (h * LOW + l, xx * CORES + c)

    x_peers = [device(hi, lo, turn(x, j, xs), core) for j in range(1, xs)]
    pair = hi + 1 - 2 * lax.rem(hi, 2)
    inward = highs - 1 - hi
    inside = jnp.logical_and(hi > 0, hi < highs - 1)
    pair_peer = device(pair, lo, x, core)
    inward_peer = device(inward, lo, x, core)
    hi_sources = [pair, 2 - hi // 2, (highs - 1) * (1 - hi // 2)]
    lo_peer = device(hi, other_lo, x, core)
    sibling = device(hi, lo, x, other_core)

    def block(s, h, far, xx, c, at=None):
        at = hi if at is None else at
        near, away = lax.rem(h + at, 2), lax.rem(h // 2 + at // 2, 2)
        r = pl.multiple_of((away * highs + far * 2 + near) * pos, pos)
        f = pl.multiple_of((xx * CORES + c) * feat, feat)
        return mem.at[s, pl.ds(r, pos), pl.ds(f, feat)]

    def slot(h, l, xx):
        return (h * LOW + l) * xs + xx

    def st_block(s, xx, c):
        return st.at[s, :, pl.ds(pl.multiple_of((xx * CORES + c) * feat, feat), feat)]

    counter = [2]
    waits = []
    traced = [set(), set()]

    def remote(src, dst, sem, recv, dev):
        return pltpu.make_async_remote_copy(
            src_ref=src, dst_ref=dst, send_sem=send_sem.at[sem], recv_sem=recv,
            device_id=dev, device_id_type=MESH,
        )

    def send(src, dst, recv, dev, like, keep=True):
        sem = counter[0]
        counter[0] += 1
        remote(src, dst, sem, recv, dev).start()
        if keep:
            waits.append((like, sem))
        return sem

    def sent(like, sem):
        remote(like, like, sem, recv_ici.at[0, 0], sibling).wait_send()

    def like_block():
        return block(0, 0, 0, 0, 0)

    def like_blocks(n):
        return mem.at[:, :n * pos * feat // (seqs * depth), :]

    def send_block(src, dst, recv, dev, sem, *key):
        traced[sem].add(key)
        remote(src, dst, sem, recv, dev).start()

    def send_own(s, h, xx, dev, at, sem, *key):
        send_block(block(s, h, 0, xx, core), block(s, h, 0, xx, core, at),
                   recv_ici.at[s, slot(h, lo, xx)], dev, sem, "own", s, *key)

    def send_inward(s, h, xx, *key):
        @pl.when(inside)
        def _():
            send_own(s, h, xx, inward_peer, inward, 1, *key)

    def send_low(s, h, xx, *key):
        send_block(block(s, h, 0, xx, core), block(s, h, 1, xx, core),
                   recv_ici.at[s, slot(h, lo, xx)], lo_peer, 0, "low", s, *key)

    def send_over(s, h, far, away, xx, *key):
        ref = block(s, h, far, xx, core)
        send_block(ref, ref, recv_d2d.at[s, away], sibling, 0, "over", s, far, *key)

    def arrived(s, h, l, xx):
        ref = like_block()
        remote(ref, ref, 0, recv_ici.at[s, slot(h, l, xx)], sibling).wait_recv()

    st_sends = [[], []]

    def low_first(s):
        send_low(s, hi, x, "first")

    def across_first(s):
        for j, dev in enumerate(x_peers):
            send_own(s, hi, x, dev, hi, 0, "across", j)

    def high_first(s):
        send_own(s, hi, x, pair_peer, pair, 0, "first")
        send_inward(s, hi, x, "first")

    def over_first(s):
        send_over(s, hi, 0, 0, x, "first")

    def state_sends(s):
        ref = st_block(s, x, core)
        for dev in x_peers:
            st_sends[s].append(send(ref, ref, st_ici.at[s, x], dev, None, False))
        st_sends[s].append(send(ref, ref, st_d2d.at[s, x], sibling, None, False))

    def forward_x(s):
        for j in range(1, xs):
            xx = turn(x, j, xs)
            arrived(s, hi, lo, xx)
            send_own(s, hi, xx, pair_peer, pair, 0, j)
            send_inward(s, hi, xx, j)
            send_low(s, hi, xx, j)
            send_over(s, hi, 0, 0, xx, j)

    high_order = [(0, 0), (0, 1), (1, 0), (1, 1), (2, 0), (2, 1)]
    low_order = [(None, j) for j in range(xs)] + high_order

    def forward_line(s, i):
        k, j = high_order[i]
        h, xx = hi_sources[k], turn(x, j, xs)
        arrived(s, h, lo, xx)
        send_own(s, h, xx, inward_peer if k == 0 else pair_peer, inward if k == 0 else pair, 1, "high", i)

    def forward_out(s, i):
        k, j = high_order[i]
        h, xx = hi_sources[k], turn(x, j, xs)
        send_low(s, h, xx, "high", i)
        send_over(s, h, 0, int(k > 0), xx, "high", i)

    def await_high(s, i):
        k, j = high_order[i]
        arrived(s, hi_sources[k], lo, turn(x, j, xs))

    def forward_low(s, i):
        k, j = low_order[i]
        h, xx = hi if k is None else hi_sources[k], turn(x, j, xs)
        arrived(s, h, other_lo, xx)
        send_over(s, h, 1, int(k is not None and k > 0), xx, i)

    def forward_states(s):
        for j in range(1, xs):
            xx = turn(x, j, xs)
            ref = st_block(s, xx, core)
            remote(ref, ref, 0, st_ici.at[s, xx], sibling).wait_recv()
            st_sends[s].append(send(ref, ref, st_d2d.at[s, xx], sibling, None, False))

    def finish_states(s):
        for xx in range(xs):
            ref = st_block(s, xx, other_core)
            remote(ref, ref, 0, st_d2d.at[s, xx], sibling).wait_recv()
        for sem in st_sends[s]:
            sent(st_block(s, x, core), sem)

    def finish_memory(s, away):
        ref = mem.at[s, :highs * pos, :xs * feat]
        remote(ref, ref, 0, recv_d2d.at[s, away], sibling).wait_recv()

    def steps(n, body, plan=()):
        plan = dict(plan)
        assert all(t < n for t in plan)

        @pl.loop(0, n)
        def _(i):
            for t, events in plan.items():
                @pl.when(i == t)
                def _(events=events):
                    do(*events)

            body(i)

    def do(*events):
        for fn, *args in events:
            if fn.__name__ in ("mid", "tip"):
                fn(*args)
            else:
                with scope("_".join([fn.__name__] + [str(a) for a in args])):
                    fn(*args)

    def normalize(s):
        part[s] = st[s, :, pl.ds(pl.multiple_of(tensor * feat, feat), feat)].astype(F32)

        @pl.loop(0, rows // SUB)
        def _(i):
            some = pl.ds(pl.multiple_of(i * SUB, SUB), SUB)
            total = jnp.zeros((SUB, LANES), F32)
            for g in range(depth // LANES):
                cols = slice(g * LANES, (g + 1) * LANES)
                xf = st[s, some, cols].astype(F32)
                total += xf * xf
                st[s, some, cols] = (xf * gain_ref[:, cols]).astype(BF16)
            squares[some, :] = total

        mean = jnp.sum(squares[...], axis=-1, keepdims=True) * (1.0 / depth)
        scale = lax.rsqrt(mean + 1e-06) * (HEAD_DIM ** -0.5)
        squares[...] = jnp.broadcast_to(scale, squares.shape)

    def query(s, plan):
        def body(i):
            cols = pl.ds(pl.multiple_of(i * TILE, TILE), TILE)
            full = jnp.dot(st[s], wq[:, cols], preferred_element_type=F32)
            scale = squares[...]
            q[s, :, cols] = (full * jnp.concatenate([scale] * (TILE // LANES), axis=1)).astype(BF16)

        steps(inner // TILE, body, plan)

    half = highs * pos

    def keyvalue(s, far, plan):
        def body(i):
            cols = pl.ds(pl.multiple_of(i * WIDE, WIDE), WIDE)
            full = jnp.dot(mem[s, far * half:(far + 1) * half], wkv[:, cols], preferred_element_type=F32)
            kv[far * half:(far + 1) * half, cols] = full.astype(BF16)

        steps(2 * inner // WIDE, body, plan)

    def attention(s, plan):
        lane = lax.broadcasted_iota(jnp.int32, (1, 2 * HEAD_DIM), 1)
        first = lane < HEAD_DIM

        def body(step):
            places = [pl.multiple_of((step * PAIRS + u) * 2 * HEAD_DIM, 2 * HEAD_DIM) for u in range(PAIRS)]
            scores, probs = [], []
            for c in places:
                qp, kp = q[s, :, pl.ds(c, 2 * HEAD_DIM)], kv[:, pl.ds(c, 2 * HEAD_DIM)]
                for mine in (first, jnp.logical_not(first)):
                    qh = jnp.where(mine, qp, jnp.zeros_like(qp))
                    scores.append(lax.dot_general(
                        qh, kp, (((1,), (1,)), ((), ())), preferred_element_type=F32
                    ))
            for one in scores:
                top = jnp.max(one, axis=-1, keepdims=True)
                probs.append(jnp.exp(one - top).astype(BF16))
            for u, c in enumerate(places):
                vp = kv[:, pl.ds(inner + c, 2 * HEAD_DIM)]
                both = jnp.concatenate([vp, jnp.ones_like(vp)], axis=1)
                outs = [jnp.dot(probs[2 * u + e], both, preferred_element_type=F32) for e in range(2)]
                total = jnp.where(first, outs[0][:, :2 * HEAD_DIM], outs[1][:, :2 * HEAD_DIM])
                sums = jnp.where(first, outs[0][:, 2 * HEAD_DIM:], outs[1][:, 2 * HEAD_DIM:])
                ctx[:, pl.ds(c, 2 * HEAD_DIM)] = (total / sums).astype(BF16)

        steps(inner // (2 * HEAD_DIM * PAIRS), body, plan)

    cuts = [slice(i, i + min(WIDE, feat)) for i in range(0, feat, min(WIDE, feat))]

    pieces = [slice(i, i + min(TILE, feat)) for i in range(0, feat, min(TILE, feat))]

    def product(t, c):
        cols = pl.ds(pl.multiple_of(t * feat + c.start, LANES), c.stop - c.start)
        return jnp.dot(ctx[...], wo[:, cols], preferred_element_type=F32)

    def output(s):
        order = [turn(x, j, xs) for j in range(1, xs)] + [x]
        last = xs - 1

        def over(j):
            for c in cuts:
                pd[s, j, :, c] = product(order[j] * CORES + other_core, c).astype(BF16)

        def over_send(j):
            send(pd.at[s, j], rd.at[s, j], pd_sem.at[s, j], sibling, lambda: pd.at[0, 0])

        def back(j):
            remote(pd.at[s, j], rd.at[s, j], 0, pd_sem.at[s, j], sibling).wait_recv()

        for j in range(last):
            over(j)
            over_send(j)
            for c in cuts:
                px[s, j, :, c] = product(order[j] * CORES + core, c).astype(BF16)
            if s < seqs - 1:
                over(last)
            back(j)
            for i, c in enumerate(pieces):
                px[s, j, :, c] = (px[s, j, :, c].astype(F32) + rd[s, j, :, c].astype(F32)).astype(BF16)
                send(px.at[s, j, :, c], rx.at[s, j, :, c], px_sem.at[s, j, i], x_peers[j],
                     lambda c=c: pd.at[0, 0, :, c])
        if s == seqs - 1:
            over(last)
        over_send(last)
        for c in cuts:
            part[s, :, c] += product(tensor, c)
        back(last)
        part[s] += rd[s, last].astype(F32)

    def out_copy(s, i, c):
        return pltpu.make_async_copy(q.at[s, :, c], out_hbm.at[s, :, c], out_sem.at[s, i])

    def finish(s):
        for i, c in enumerate(pieces):
            total = part[s, :, c]
            for j in range(xs - 1):
                remote(px.at[s, j, :, c], rx.at[s, j, :, c], 0, px_sem.at[s, j, i], sibling).wait_recv()
                total += rx[s, j, :, c].astype(F32)
            q[s, :, c] = total.astype(BF16)
            out_copy(s, i, c).start()

    groups = 2 * inner // LANES
    size = CHUNK * groups
    chunks = depth // CHUNK
    slots = staged.shape[0]

    def stage(i, slot):
        src = wkv_hbm.at[pl.ds(pl.multiple_of(i * size, size), size), :]
        return pltpu.make_async_copy(src, staged.at[slot], stage_sem.at[slot])

    def spread(plan):
        span = SUB * groups
        a = lax.broadcasted_iota(jnp.int32, (span, span), 0)
        b = lax.broadcasted_iota(jnp.int32, (span, span), 1)
        swap = (b == lax.rem(a, SUB) * groups + a // SUB).astype(F32).astype(BF16)

        def body(i):
            slot = lax.rem(i, slots)
            stage(i, slot).wait()
            for m in range(CHUNK // (2 * SUB)):
                r = m * 2 * span
                both = jnp.concatenate(
                    [staged[slot, r:r + span, :], staged[slot, r + span:r + 2 * span, :]], axis=1
                )
                moved = jnp.dot(swap, both, preferred_element_type=F32).astype(BF16)
                d = pl.multiple_of(i * CHUNK + m * 2 * SUB, 2 * SUB)
                for g in range(groups):
                    col = (g % 2) * inner + (g // 2) * LANES
                    piece = moved[g * SUB:(g + 1) * SUB]
                    wkv[pl.ds(d, SUB), col:col + LANES] = piece[:, :LANES]
                    wkv[pl.ds(d + SUB, SUB), col:col + LANES] = piece[:, LANES:]

            @pl.when(i + slots < chunks)
            def _():
                stage(i + slots, slot).start()

        steps(chunks, body, plan)

    loads = [
        pltpu.make_async_copy(mem_hbm.at[0], block(0, hi, 0, x, core), load_sem.at[0]),
        pltpu.make_async_copy(st_hbm.at[0], st_block(0, x, core), load_sem.at[1]),
        pltpu.make_async_copy(mem_hbm.at[1], block(1, hi, 0, x, core), load_sem.at[2]),
        pltpu.make_async_copy(st_hbm.at[1], st_block(1, x, core), load_sem.at[3]),
    ]
    weights = [
        pltpu.make_async_copy(wq_hbm, wq, load_sem.at[4]),
        pltpu.make_async_copy(wo_hbm, wo, load_sem.at[5]),
    ]
    for copy in loads:
        copy.start()
    barrier = pltpu.get_barrier_semaphore()
    peers = x_peers + [pair_peer, lo_peer, sibling]
    for peer in peers:
        pl.semaphore_signal(barrier, inc=1, device_id=peer, device_id_type=MESH)

    @pl.when(inside)
    def _():
        pl.semaphore_signal(barrier, inc=1, device_id=inward_peer, device_id_type=MESH)

    for i in range(slots):
        stage(i, i).start()
    with scope("barrier"):
        pl.semaphore_wait(barrier, len(peers) + lax.rem(hi + hi // 2, 2))
    with scope("load0"):
        loads[0].wait()
    across_first(0)
    low_first(0)
    high_first(0)
    over_first(0)
    with scope("load1"):
        loads[1].wait()
    state_sends(0)
    loads[2].wait()
    low_first(1)
    high_first(1)
    across_first(1)
    over_first(1)
    loads[3].wait()
    state_sends(1)

    outside = jnp.logical_not(inside)

    def load(i): weights[i].start()

    def fx(s): forward_x(s)

    def fl(s, i): forward_low(s, i)

    def mid(*events):
        @pl.when(inside)
        def _():
            do(*events)

    def tip(*events):
        @pl.when(outside)
        def _():
            do(*events)

    def ml(s, i): forward_line(s, i)

    def fo(s, i): forward_out(s, i)

    def fi(s, i):
        forward_line(s, i)
        forward_out(s, i)

    def ft(s, i):
        await_high(s, i)
        forward_out(s, i)

    with scope("spread"):
        spread({
            6: [(fx, 0), (fl, 0, 0), (mid, (fi, 0, 0), (ml, 0, 2)), (tip, (ft, 0, 0))],
            10: [(load, 0)],
            12: [(fl, 0, 1), (mid, (fi, 0, 1), (fo, 0, 2), (fi, 0, 3)), (tip, (ft, 0, 1))],
        })
    do((load, 1), (mid, (fi, 0, 4)), (tip, (ft, 0, 2)), (fl, 0, 2), (mid, (fi, 0, 5)), (tip, (ft, 0, 3)), (fl, 0, 3))
    with scope("finmem00"):
        finish_memory(0, 0)
    with scope("kv00"):
        keyvalue(0, 0, {
            0: [(forward_states, 0)],
            1: [(tip, (ft, 0, 4)), (fl, 0, 4)],
            3: [(tip, (ft, 0, 5)), (fx, 1), (fl, 0, 5)],
        })
    with scope("finst0"):
        finish_states(0)
    with scope("norm0"):
        normalize(0)
    with scope("wq"):
        weights[0].wait()
    with scope("query0"):
        query(0, {
            1: [(fl, 0, 6)],
            2: [(mid, (fi, 1, 0), (ml, 1, 2)), (tip, (ft, 1, 0))],
        })
    do((mid, (fi, 1, 1), (fo, 1, 2), (fi, 1, 3)), (tip, (ft, 1, 1)), (fl, 0, 7))
    with scope("finmem01"):
        finish_memory(0, 1)
    with scope("kv01"):
        keyvalue(0, 1, {
            1: [(fl, 1, 0), (tip, (ft, 1, 2)), (mid, (fi, 1, 4))],
            2: [(forward_states, 1)],
            3: [(fl, 1, 1), (mid, (fi, 1, 5)), (tip, (ft, 1, 3))],
        })
    with scope("att0"):
        attention(0, {
            0: [(fl, 1, 2)],
            1: [(tip, (ft, 1, 4))],
        })
    with scope("finst1"):
        finish_states(1)
    with scope("norm1"):
        normalize(1)
    with scope("query1"):
        query(1, {
            0: [(fl, 1, 3), (tip, (ft, 1, 5))],
            2: [(fl, 1, 4)],
        })
    weights[1].wait()
    with scope("output0"):
        output(0)
    do((fl, 1, 5))
    with scope("finmem10"):
        finish_memory(1, 0)
    with scope("kv10"):
        keyvalue(1, 0, {1: [(fl, 1, 6)], 3: [(fl, 1, 7)]})
    with scope("finmem11"):
        finish_memory(1, 1)
    with scope("kv11"):
        keyvalue(1, 1, {})
    with scope("att1"):
        attention(1, {})
    with scope("output1"):
        output(1)
    with scope("finish0"):
        finish(0)
    with scope("finish1"):
        finish(1)
    assert [len(t) for t in traced] == [54, 16], [len(t) for t in traced]
    with scope("end"):
        for like, sem in waits:
            sent(like(), sem)
        for s in range(seqs):
            for i, c in enumerate(pieces):
                out_copy(s, i, c).wait()
        sent(like_blocks(len(traced[0])), 0)

        @pl.when(inside)
        def _():
            sent(like_blocks(len(traced[1])), 1)


def fused(n_pipe, n_tensor, memory, states, norm_gain, w_query, w_keyvalue, w_output):
    seqs, pos, feat = memory.shape
    rows = states.shape[2]
    depth, inner = feat * n_tensor, w_query.shape[2]
    enc = pos * n_pipe
    xs, highs = n_tensor // CORES, n_pipe // LOW
    groups = 2 * inner // LANES
    weight_kv = w_keyvalue[0].reshape(depth, 2, inner // LANES, LANES)
    weight_kv = weight_kv.transpose(0, 2, 1, 3).reshape(depth * groups, LANES)
    blocks = n_pipe * xs
    tiles = feat // min(TILE, feat)
    copies = seqs * (xs + xs + xs + (xs - 1) * tiles) + 2
    any_space = pl.BlockSpec(memory_space=pl.ANY)
    in_vmem = pl.BlockSpec(memory_space=pltpu.VMEM)
    dma = pltpu.SemaphoreType.DMA
    out = pl.pallas_call(
        functools.partial(kernel, n_pipe, n_tensor),
        out_shape=jax.ShapeDtypeStruct((seqs, rows, feat), BF16),
        in_specs=[any_space, any_space, in_vmem, any_space, any_space, any_space],
        out_specs=any_space,
        scratch_shapes=[
            pltpu.VMEM((seqs, enc, depth), BF16),
            pltpu.VMEM((seqs, rows, depth), BF16),
            pltpu.VMEM((depth, inner), BF16),
            pltpu.VMEM((depth, 2 * inner), BF16),
            pltpu.VMEM((inner, depth), BF16),
            pltpu.VMEM((seqs, rows, max(inner, feat)), BF16),
            pltpu.VMEM((enc, 2 * inner), BF16),
            pltpu.VMEM((rows, inner), BF16),
            pltpu.VMEM((seqs, xs, rows, feat), BF16),
            pltpu.VMEM((seqs, xs, rows, feat), BF16),
            pltpu.VMEM((seqs, xs - 1, rows, feat), BF16),
            pltpu.VMEM((seqs, xs - 1, rows, feat), BF16),
            pltpu.VMEM((seqs, rows, feat), F32),
            pltpu.VMEM((SLOTS, CHUNK * groups, LANES), BF16),
            pltpu.VMEM((rows, LANES), F32),
            dma((6,)),
            dma((SLOTS,)),
            dma((copies,)),
            dma((seqs, blocks)),
            dma((seqs, LOW)),
            dma((seqs, xs)),
            dma((seqs, xs)),
            dma((seqs, xs)),
            dma((seqs, xs - 1, tiles)),
            dma((seqs, tiles)),
        ],
        compiler_params=pltpu.CompilerParams(
            collective_id=0, has_side_effects=True, vmem_limit_bytes=67_000_000
        ),
    )(memory, states[0], norm_gain, w_query[0], weight_kv, w_output[0])
    return out[None]


def per_device(memory, states, norm_gain, w_query, w_keyvalue, w_output):
    whole_states = lax.all_gather(states[0], "tensor", axis=2, tiled=True)
    xf = whole_states.astype(jnp.float32)
    scale = lax.rsqrt(jnp.mean(xf * xf, axis=-1, keepdims=True) + 1e-06)
    normed = (xf * scale * norm_gain[0]).astype(jnp.bfloat16)
    weight_q = w_query[0]
    local_inner = weight_q.shape[1]
    weight_kv = w_keyvalue[0].reshape(w_keyvalue.shape[1], 2 * local_inner)
    weight_o = w_output[0]
    seqs = normed.shape[0]
    dec_rows = normed.shape[1]
    local_heads = local_inner // HEAD_DIM
    query = jnp.einsum("btd,de->bte", normed, weight_q, preferred_element_type=jnp.float32).astype(
        jnp.bfloat16
    )
    gathered = lax.all_gather(memory, "pipe", axis=1, tiled=True)
    gathered = lax.all_gather(gathered, "tensor", axis=2, tiled=True)
    keyvalue = jnp.einsum(
        "bpd,de->bpe", gathered, weight_kv, preferred_element_type=jnp.float32
    ).astype(jnp.bfloat16)
    enc_rows = keyvalue.shape[1]
    keys = keyvalue[:, :, :local_inner].reshape(seqs, enc_rows, local_heads, HEAD_DIM)
    values = keyvalue[:, :, local_inner:].reshape(seqs, enc_rows, local_heads, HEAD_DIM)
    heads_q = query.reshape(seqs, dec_rows, local_heads, HEAD_DIM)
    scores = jnp.einsum(
        "bqhd,bkhd->bhqk", heads_q, keys, preferred_element_type=jnp.float32
    ) / jnp.sqrt(jnp.float32(HEAD_DIM))
    probs = jax.nn.softmax(scores, axis=-1).astype(jnp.bfloat16)
    context = jnp.einsum(
        "bhqk,bkhd->bqhd", probs, values, preferred_element_type=jnp.float32
    ).astype(jnp.bfloat16)
    context = context.reshape(seqs, dec_rows, local_inner)
    partial_terms = jnp.einsum("bte,ed->btd", context, weight_o, preferred_element_type=jnp.float32)
    branch = lax.psum_scatter(partial_terms, "tensor", scatter_dimension=2, tiled=True)
    result = (states[0].astype(jnp.float32) + branch).astype(jnp.bfloat16)
    return result[None]


def solution(mesh):
    in_specs = (
        P(None, "pipe", "tensor"),
        P("pipe", None, None, "tensor"),
        P("pipe", None),
        P("pipe", None, "tensor"),
        P("pipe", None, None, "tensor"),
        P("pipe", "tensor", None),
    )
    out_specs = P("pipe", None, None, "tensor")
    n_pipe, n_tensor = mesh.shape["pipe"], mesh.shape["tensor"]
    even = n_pipe % LOW == 0 and n_tensor % CORES == 0 and n_pipe > LOW and n_tensor > CORES
    even = even and n_pipe // LOW == 4 and n_tensor // CORES == 2
    even = even and n_pipe // LOW == 4 and n_tensor // CORES == 2
    body = per_device
    if even and copies_per_sequence(n_pipe, n_tensor) <= MAX_COPIES:
        body = functools.partial(fused, n_pipe, n_tensor)
    return jax.shard_map(
        body, mesh=mesh, in_specs=in_specs, out_specs=out_specs, check_vma=False
    )
```

```python
import functools

import jax
import jax.numpy as jnp
from jax import lax
from jax.experimental import pallas as pl
from jax.experimental.pallas import tpu as pltpu
from jax.sharding import PartitionSpec as P

HEAD_DIM = 64
CORES = 2
LOW = 2
TILE = 256
WIDE = 512
MAX_COPIES = 100
LANES = 128
SUB = 16
CHUNK = 256
SLOTS = 3
PAIRS = 4
MESH = pl.DeviceIdType.MESH
F32 = jnp.float32
BF16 = jnp.bfloat16


def copies_per_sequence(n_pipe, n_tensor):
    xs, highs = n_tensor // CORES, n_pipe // LOW
    return 4 * n_pipe * xs + (xs - 1) * highs


def kernel(
    n_pipe, n_tensor,
    mem_hbm, st_hbm, gain_ref, wq_hbm, wkv_hbm, wo_hbm, out_hbm,
    mem, st, wq, wkv, wo, q, kv, pd, rd, px, rx, part, staged, squares,
    load_sem, stage_sem, send_sem, recv_ici, recv_d2d, st_ici, st_d2d, pd_sem, px_sem, out_sem,
):
    xs, highs = n_tensor // CORES, n_pipe // LOW
    seqs, enc, depth = mem.shape
    rows = st.shape[1]
    pos = enc // n_pipe
    feat = depth // n_tensor
    inner = wq.shape[1]
    pipe = lax.axis_index("pipe")
    tensor = lax.axis_index("tensor")
    hi, lo = pipe // LOW, pipe % LOW
    x, core = tensor // CORES, tensor % CORES
    other_lo, other_core = 1 - lo, 1 - core
    scope = jax.named_scope

    def turn(a, k, n):
        return lax.rem(a + k, n)

    def device(h, l, xx, c):
        return (h * LOW + l, xx * CORES + c)

    x_peers = [device(hi, lo, turn(x, j, xs), core) for j in range(1, xs)]
    pair = hi + 1 - 2 * lax.rem(hi, 2)
    inward = highs - 1 - hi
    inside = jnp.logical_and(hi > 0, hi < highs - 1)
    pair_peer = device(pair, lo, x, core)
    inward_peer = device(inward, lo, x, core)
    hi_sources = [pair, 2 - hi // 2, (highs - 1) * (1 - hi // 2)]
    lo_peer = device(hi, other_lo, x, core)
    sibling = device(hi, lo, x, other_core)

    def block(s, h, far, xx, c, at=None):
        at = hi if at is None else at
        near, away = lax.rem(h + at, 2), lax.rem(h // 2 + at // 2, 2)
        r = pl.multiple_of((away * highs + far * 2 + near) * pos, pos)
        f = pl.multiple_of((xx * CORES + c) * feat, feat)
        return mem.at[s, pl.ds(r, pos), pl.ds(f, feat)]

    def slot(h, l, xx):
        return (h * LOW + l) * xs + xx

    def st_block(s, xx, c):
        return st.at[s, :, pl.ds(pl.multiple_of((xx * CORES + c) * feat, feat), feat)]

    counter = [2]
    waits = []
    traced = [set(), set()]

    def remote(src, dst, sem, recv, dev):
        return pltpu.make_async_remote_copy(
            src_ref=src, dst_ref=dst, send_sem=send_sem.at[sem], recv_sem=recv,
            device_id=dev, device_id_type=MESH,
        )

    def send(src, dst, recv, dev, like, keep=True):
        sem = counter[0]
        counter[0] += 1
        remote(src, dst, sem, recv, dev).start()
        if keep:
            waits.append((like, sem))
        return sem

    def sent(like, sem):
        remote(like, like, sem, recv_ici.at[0, 0], sibling).wait_send()

    def like_block():
        return block(0, 0, 0, 0, 0)

    def like_blocks(n):
        return mem.at[:, :n * pos * feat // (seqs * depth), :]

    def send_block(src, dst, recv, dev, sem, *key):
        traced[sem].add(key)
        remote(src, dst, sem, recv, dev).start()

    def send_own(s, h, xx, dev, at, sem, *key):
        send_block(block(s, h, 0, xx, core), block(s, h, 0, xx, core, at),
                   recv_ici.at[s, slot(h, lo, xx)], dev, sem, "own", s, *key)

    def send_inward(s, h, xx, *key):
        @pl.when(inside)
        def _():
            send_own(s, h, xx, inward_peer, inward, 1, *key)

    def send_low(s, h, xx, *key):
        send_block(block(s, h, 0, xx, core), block(s, h, 1, xx, core),
                   recv_ici.at[s, slot(h, lo, xx)], lo_peer, 0, "low", s, *key)

    def send_over(s, h, far, away, xx, *key):
        ref = block(s, h, far, xx, core)
        send_block(ref, ref, recv_d2d.at[s, away], sibling, 0, "over", s, far, *key)

    def arrived(s, h, l, xx):
        ref = like_block()
        remote(ref, ref, 0, recv_ici.at[s, slot(h, l, xx)], sibling).wait_recv()

    st_sends = [[], []]

    def low_first(s):
        send_low(s, hi, x, "first")

    def across_first(s):
        for j, dev in enumerate(x_peers):
            send_own(s, hi, x, dev, hi, 0, "across", j)

    def high_first(s):
        send_own(s, hi, x, pair_peer, pair, 0, "first")
        send_inward(s, hi, x, "first")

    def over_first(s):
        send_over(s, hi, 0, 0, x, "first")

    def state_sends(s):
        ref = st_block(s, x, core)
        for dev in x_peers:
            st_sends[s].append(send(ref, ref, st_ici.at[s, x], dev, None, False))
        st_sends[s].append(send(ref, ref, st_d2d.at[s, x], sibling, None, False))

    def forward_x(s):
        for j in range(1, xs):
            xx = turn(x, j, xs)
            arrived(s, hi, lo, xx)
            send_own(s, hi, xx, pair_peer, pair, 0, j)
            send_inward(s, hi, xx, j)
            send_low(s, hi, xx, j)
            send_over(s, hi, 0, 0, xx, j)

    high_order = [(0, 0), (0, 1), (1, 0), (1, 1), (2, 0), (2, 1)]
    SIDEWAYS = 3
    low_order = [(None, j) for j in range(xs)] + high_order

    def forward_line(s, i):
        k, j = high_order[i]
        h, xx = hi_sources[k], turn(x, j, xs)
        arrived(s, h, lo, xx)
        send_own(s, h, xx, inward_peer if k == 0 else pair_peer, inward if k == 0 else pair, 1, "high", i)

    def forward_out(s, i):
        k, j = high_order[i]
        h, xx = hi_sources[k], turn(x, j, xs)
        if (s, i) != (seqs - 1, SIDEWAYS):
            send_low(s, h, xx, "high", i)
        send_over(s, h, 0, int(k > 0), xx, "high", i)

    def await_high(s, i):
        k, j = high_order[i]
        arrived(s, hi_sources[k], lo, turn(x, j, xs))

    def forward_low(s, i):
        k, j = low_order[i]
        h, xx = hi if k is None else hi_sources[k], turn(x, j, xs)
        arrived(s, h, other_lo, xx)
        if s == seqs - 1 and k == high_order[SIDEWAYS][0] and j == 0:
            ref = block(s, h, 1, xx, core)
            send_block(ref, ref, recv_ici.at[s, slot(h, other_lo, xx)], x_peers[0], 0, "sideways", s)
        send_over(s, h, 1, int(k is not None and k > 0), xx, i)

    def forward_states(s):
        for j in range(1, xs):
            xx = turn(x, j, xs)
            ref = st_block(s, xx, core)
            remote(ref, ref, 0, st_ici.at[s, xx], sibling).wait_recv()
            st_sends[s].append(send(ref, ref, st_d2d.at[s, xx], sibling, None, False))

    def finish_states(s):
        for j in range(int(s == seqs - 1), xs):
            xx = turn(x, j, xs)
            ref = st_block(s, xx, other_core)
            remote(ref, ref, 0, st_d2d.at[s, xx], sibling).wait_recv()
        for sem in st_sends[s]:
            sent(st_block(s, x, core), sem)

    def finish_memory(s, away):
        ref = mem.at[s, :highs * pos, :xs * feat]
        remote(ref, ref, 0, recv_d2d.at[s, away], sibling).wait_recv()

    def steps(n, body, plan=()):
        plan = dict(plan)
        assert all(t < n for t in plan)

        @pl.loop(0, n)
        def _(i):
            for t, events in plan.items():
                @pl.when(i == t)
                def _(events=events):
                    do(*events)

            body(i)

    def do(*events):
        for fn, *args in events:
            if fn.__name__ in ("mid", "tip"):
                fn(*args)
            else:
                with scope("_".join([fn.__name__] + [str(a) for a in args])):
                    fn(*args)

    def set_scale(s):
        mean = jnp.sum(squares[s], axis=-1, keepdims=True) * (1.0 / depth)
        scale = lax.rsqrt(mean + 1e-06) * (HEAD_DIM ** -0.5)
        squares[s] = jnp.broadcast_to(scale, (rows, LANES))

    def normalize(s):
        part[s] = st[s, :, pl.ds(pl.multiple_of(tensor * feat, feat), feat)].astype(F32)

        @pl.loop(0, rows // SUB)
        def _(i):
            some = pl.ds(pl.multiple_of(i * SUB, SUB), SUB)
            total = jnp.zeros((SUB, LANES), F32)
            for g in range(depth // LANES):
                cols = slice(g * LANES, (g + 1) * LANES)
                xf = st[s, some, cols].astype(F32)
                total += xf * xf
                st[s, some, cols] = (xf * gain_ref[:, cols]).astype(BF16)
            squares[s, some, :] = total

        set_scale(s)

    def query(s, plan):
        def body(i):
            cols = pl.ds(pl.multiple_of(i * TILE, TILE), TILE)
            full = jnp.dot(st[s], wq[:, cols], preferred_element_type=F32)
            scale = squares[s]
            q[s, :, cols] = (full * jnp.concatenate([scale] * (TILE // LANES), axis=1)).astype(BF16)

        steps(inner // TILE, body, plan)

    def chip_features(xx, c):
        return pl.multiple_of((xx * CORES + c) * feat, feat)

    def early_query(s, plan):
        ref = st_block(s, x, other_core)
        remote(ref, ref, 0, st_d2d.at[s, x], sibling).wait_recv()

        @pl.loop(0, rows // SUB)
        def _(i):
            some = pl.ds(pl.multiple_of(i * SUB, SUB), SUB)
            total = jnp.zeros((SUB, LANES), F32)
            for c in range(CORES):
                for g in range(feat // LANES):
                    cols = pl.ds(pl.multiple_of(chip_features(x, c) + g * LANES, LANES), LANES)
                    xf = st[s, some, cols].astype(F32)
                    total += xf * xf
                    pd[s, c, some, g * LANES:(g + 1) * LANES] = (xf * gain_ref[:, cols]).astype(BF16)
            squares[s, some, :] = total

        def body(i):
            cols = pl.ds(pl.multiple_of(i * WIDE, WIDE), WIDE)
            part[s, :, cols] = sum(
                jnp.dot(pd[s, c], wq[pl.ds(chip_features(x, c), feat), cols], preferred_element_type=F32)
                for c in range(CORES)
            )

        steps(inner // WIDE, body, plan)

    def late_query(s, plan):
        xx = turn(x, 1, xs)

        @pl.loop(0, rows // SUB)
        def _(i):
            some = pl.ds(pl.multiple_of(i * SUB, SUB), SUB)
            total = squares[s, some, :]
            for c in range(CORES):
                for g in range(feat // LANES):
                    cols = pl.ds(pl.multiple_of(chip_features(xx, c) + g * LANES, LANES), LANES)
                    xf = st[s, some, cols].astype(F32)
                    total += xf * xf
                    st[s, some, cols] = (xf * gain_ref[:, cols]).astype(BF16)
            squares[s, some, :] = total

        set_scale(s)

        def body(i):
            cols = pl.ds(pl.multiple_of(i * WIDE, WIDE), WIDE)
            mine = pl.ds(chip_features(xx, 0), CORES * feat)
            full = part[s, :, cols] + jnp.dot(st[s, :, mine], wq[mine, cols], preferred_element_type=F32)
            q[s, :, cols] = (full * jnp.concatenate([squares[s]] * (WIDE // LANES), axis=1)).astype(BF16)

        steps(inner // WIDE, body, plan)
        part[s] = st[s, :, pl.ds(pl.multiple_of(tensor * feat, feat), feat)].astype(F32)

    half = highs * pos

    def keyvalue(s, far, plan, per=1):
        def body(i):
            for u in range(per):
                cols = pl.ds(pl.multiple_of((i * per + u) * WIDE, WIDE), WIDE)
                full = jnp.dot(mem[s, far * half:(far + 1) * half], wkv[:, cols], preferred_element_type=F32)
                kv[far * half:(far + 1) * half, cols] = full.astype(BF16)

        steps(2 * inner // (WIDE * per), body, plan)

    def attention(s, plan):
        lane = lax.broadcasted_iota(jnp.int32, (1, 2 * HEAD_DIM), 1)
        first = lane < HEAD_DIM

        def body(step):
            places = [pl.multiple_of((step * PAIRS + u) * 2 * HEAD_DIM, 2 * HEAD_DIM) for u in range(PAIRS)]
            scores, probs = [], []
            for c in places:
                qp, kp = q[s, :, pl.ds(c, 2 * HEAD_DIM)], kv[:, pl.ds(c, 2 * HEAD_DIM)]
                for mine in (first, jnp.logical_not(first)):
                    qh = jnp.where(mine, qp, jnp.zeros_like(qp))
                    scores.append(lax.dot_general(
                        qh, kp, (((1,), (1,)), ((), ())), preferred_element_type=F32
                    ))
            for one in scores:
                top = jnp.max(one, axis=-1, keepdims=True)
                probs.append(jnp.exp(one - top).astype(BF16))
            for u, c in enumerate(places):
                vp = kv[:, pl.ds(inner + c, 2 * HEAD_DIM)]
                both = jnp.concatenate([vp, jnp.ones_like(vp)], axis=1)
                outs = [jnp.dot(probs[2 * u + e], both, preferred_element_type=F32) for e in range(2)]
                total = jnp.where(first, outs[0][:, :2 * HEAD_DIM], outs[1][:, :2 * HEAD_DIM])
                sums = jnp.where(first, outs[0][:, 2 * HEAD_DIM:], outs[1][:, 2 * HEAD_DIM:])
                q[s, :, pl.ds(c, 2 * HEAD_DIM)] = (total / sums).astype(BF16)

        steps(inner // (2 * HEAD_DIM * PAIRS), body, plan)

    cuts = [slice(i, i + min(WIDE, feat)) for i in range(0, feat, min(WIDE, feat))]

    pieces = [slice(i, i + min(TILE, feat)) for i in range(0, feat, min(TILE, feat))]

    def product(s, t, c):
        cols = pl.ds(pl.multiple_of(t * feat + c.start, LANES), c.stop - c.start)
        return jnp.dot(q[s, :, :inner], wo[:, cols], preferred_element_type=F32)

    order = [turn(x, j, xs) for j in range(1, xs)] + [x]
    last = xs - 1
    whole = slice(0, feat)
    lead, rest = [pieces[0]], [slice(pieces[1].start, cuts[0].stop)] + cuts[1:]

    def bounds(group):
        return slice(group[0].start, group[-1].stop)

    def over(s, j, group):
        for c in group:
            pd[s, j, :, c] = product(s, order[j] * CORES + other_core, c).astype(BF16)

    def mine(s, j, group):
        for c in group:
            px[s, j, :, c] = product(s, order[j] * CORES + core, c).astype(BF16)

    def over_send(s, j, g, c):
        send(pd.at[s, j, :, c], rd.at[s, j, :, c], pd_sem.at[s, j, g], sibling, lambda: pd.at[0, 0, :, c])

    def back(s, j, g, c):
        remote(pd.at[s, j, :, c], rd.at[s, j, :, c], 0, pd_sem.at[s, j, g], sibling).wait_recv()

    def pass_on(s, g, b):
        for j in range(last):
            back(s, j, g, b)
            for i, c in enumerate(pieces):
                if b.start <= c.start < b.stop:
                    px[s, j, :, c] = (px[s, j, :, c].astype(F32) + rd[s, j, :, c].astype(F32)).astype(BF16)
                    send(px.at[s, j, :, c], rx.at[s, j, :, c], px_sem.at[s, j, i], x_peers[j],
                         lambda c=c: pd.at[0, 0, :, c])

    def output(s):
        for j in range(last):
            over(s, j, cuts)
            mine(s, j, cuts)
            over_send(s, j, 0, whole)

    def output_early(s):
        for j in range(last):
            over(s, j, lead)
            over_send(s, j, 0, bounds(lead))
            mine(s, j, lead)
            over(s, j, rest)
            over_send(s, j, 1, bounds(rest))
        pass_on(s, 0, bounds(lead))
        for j in range(last):
            mine(s, j, rest)
        pass_on(s, 1, bounds(rest))

    def output_here(s):
        over(s, last, cuts)
        over_send(s, last, 0, whole)
        for c in cuts:
            part[s, :, c] += product(s, tensor, c)

    def out_copy(s, i, c):
        return pltpu.make_async_copy(q.at[s, :, c], out_hbm.at[s, :, c], out_sem.at[s, i])

    def finish(s):
        back(s, last, 0, whole)
        for i, c in enumerate(pieces):
            part[s, :, c] += rd[s, last, :, c].astype(F32)
        for i, c in enumerate(pieces):
            total = part[s, :, c]
            for j in range(xs - 1):
                remote(px.at[s, j, :, c], rx.at[s, j, :, c], 0, px_sem.at[s, j, i], sibling).wait_recv()
                total += rx[s, j, :, c].astype(F32)
            q[s, :, c] = total.astype(BF16)
            out_copy(s, i, c).start()

    groups = 2 * inner // LANES
    size = CHUNK * groups
    chunks = depth // CHUNK
    slots = staged.shape[0]

    def stage(i, slot):
        src = wkv_hbm.at[pl.ds(pl.multiple_of(i * size, size), size), :]
        return pltpu.make_async_copy(src, staged.at[slot], stage_sem.at[slot])

    def spread(plan):
        span = SUB * groups
        a = lax.broadcasted_iota(jnp.int32, (span, span), 0)
        b = lax.broadcasted_iota(jnp.int32, (span, span), 1)
        swap = (b == lax.rem(a, SUB) * groups + a // SUB).astype(F32).astype(BF16)

        def body(i):
            slot = lax.rem(i, slots)
            stage(i, slot).wait()
            for m in range(CHUNK // (2 * SUB)):
                r = m * 2 * span
                both = jnp.concatenate(
                    [staged[slot, r:r + span, :], staged[slot, r + span:r + 2 * span, :]], axis=1
                )
                moved = jnp.dot(swap, both, preferred_element_type=F32).astype(BF16)
                d = pl.multiple_of(i * CHUNK + m * 2 * SUB, 2 * SUB)
                for g in range(groups):
                    col = (g % 2) * inner + (g // 2) * LANES
                    piece = moved[g * SUB:(g + 1) * SUB]
                    wkv[pl.ds(d, SUB), col:col + LANES] = piece[:, :LANES]
                    wkv[pl.ds(d + SUB, SUB), col:col + LANES] = piece[:, LANES:]

            @pl.when(i + slots < chunks)
            def _():
                stage(i + slots, slot).start()

        steps(chunks, body, plan)

    loads = [
        pltpu.make_async_copy(mem_hbm.at[0], block(0, hi, 0, x, core), load_sem.at[0]),
        pltpu.make_async_copy(st_hbm.at[0], st_block(0, x, core), load_sem.at[1]),
        pltpu.make_async_copy(mem_hbm.at[1], block(1, hi, 0, x, core), load_sem.at[2]),
        pltpu.make_async_copy(st_hbm.at[1], st_block(1, x, core), load_sem.at[3]),
    ]
    weights = [
        pltpu.make_async_copy(wq_hbm, wq, load_sem.at[4]),
        pltpu.make_async_copy(wo_hbm, wo, load_sem.at[5]),
    ]
    for copy in loads:
        copy.start()
    barrier = pltpu.get_barrier_semaphore()
    peers = x_peers + [pair_peer, lo_peer, sibling]
    for peer in peers:
        pl.semaphore_signal(barrier, inc=1, device_id=peer, device_id_type=MESH)

    @pl.when(inside)
    def _():
        pl.semaphore_signal(barrier, inc=1, device_id=inward_peer, device_id_type=MESH)

    for i in range(slots):
        stage(i, i).start()
    with scope("barrier"):
        pl.semaphore_wait(barrier, len(peers) + lax.rem(hi + hi // 2, 2))
    with scope("load0"):
        loads[0].wait()
    across_first(0)
    low_first(0)
    high_first(0)
    over_first(0)
    with scope("load1"):
        loads[1].wait()
    state_sends(0)
    loads[2].wait()
    low_first(1)
    high_first(1)
    across_first(1)
    over_first(1)
    loads[3].wait()
    state_sends(1)

    outside = jnp.logical_not(inside)

    def load(i): weights[i].start()

    def across(s): pass_on(s, 0, whole)

    def fx(s): forward_x(s)

    def fl(s, i): forward_low(s, i)

    def mid(*events):
        @pl.when(inside)
        def _():
            do(*events)

    def tip(*events):
        @pl.when(outside)
        def _():
            do(*events)

    def ml(s, i): forward_line(s, i)

    def fo(s, i): forward_out(s, i)

    def fi(s, i):
        forward_line(s, i)
        forward_out(s, i)

    def ft(s, i):
        await_high(s, i)
        forward_out(s, i)

    with scope("spread"):
        spread({
            6: [(fx, 0), (fl, 0, 0), (mid, (fi, 0, 0), (ml, 0, 2)), (tip, (ft, 0, 0))],
            10: [(load, 0)],
            12: [(fl, 0, 1), (mid, (fi, 0, 1), (fo, 0, 2), (fi, 0, 3)), (tip, (ft, 0, 1))],
        })
    do((load, 1), (mid, (fi, 0, 4)), (tip, (ft, 0, 2)), (fl, 0, 2))
    weights[0].wait()
    with scope("early"):
        early_query(1, {1: [(mid, (fi, 0, 5))]})
    do((fl, 0, 3), (tip, (ft, 0, 3)))
    with scope("finmem00"):
        finish_memory(0, 0)
    with scope("kv00"):
        keyvalue(0, 0, {
            0: [(forward_states, 0)],
            1: [(tip, (ft, 0, 4)), (fl, 0, 4)],
        }, 2)
    do((tip, (ft, 0, 5)), (fx, 1), (fl, 0, 5))
    with scope("finst0"):
        finish_states(0)
    with scope("norm0"):
        normalize(0)
    with scope("query0"):
        query(0, {
            1: [(fl, 0, 6)],
            2: [(mid, (fi, 1, 0), (ml, 1, 2)), (tip, (ft, 1, 0))],
        })
    do((mid, (fi, 1, 1), (fo, 1, 2), (fi, 1, 3)), (tip, (ft, 1, 1)), (fl, 0, 7))
    with scope("finmem01"):
        finish_memory(0, 1)
    with scope("kv01"):
        keyvalue(0, 1, {
            1: [(fl, 1, 0), (tip, (ft, 1, 2)), (mid, (fi, 1, 4))],
        }, 2)
    do((forward_states, 1), (fl, 1, 1))
    with scope("att0"):
        attention(0, {
            0: [(mid, (fi, 1, 5)), (tip, (ft, 1, 3)), (fl, 1, 2)],
        })
    with scope("finst1"):
        finish_states(1)
    with scope("query1"):
        late_query(1, {
            0: [(tip, (ft, 1, 4)), (fl, 1, 3)],
            1: [(tip, (ft, 1, 5))],
        })
    weights[1].wait()
    do((fl, 1, 4))
    with scope("output0"):
        output(0)
    with scope("finmem10"):
        finish_memory(1, 0)
    with scope("kv10"):
        keyvalue(1, 0, {1: [(across, 0), (fl, 1, 6)]}, 2)
    do((fl, 1, 5), (fl, 1, 7))
    with scope("finmem11"):
        finish_memory(1, 1)
    with scope("kv11"):
        keyvalue(1, 1, {}, 2)
    with scope("att1"):
        attention(1, {})
    with scope("output1"):
        output_early(1)
    with scope("here0"):
        output_here(0)
    with scope("here1"):
        output_here(1)
    with scope("finish0"):
        finish(0)
    with scope("finish1"):
        finish(1)
    assert [len(t) for t in traced] == [54, 16], [len(t) for t in traced]
    with scope("end"):
        for like, sem in waits:
            sent(like(), sem)
        for s in range(seqs):
            for i, c in enumerate(pieces):
                out_copy(s, i, c).wait()
        sent(like_blocks(len(traced[0])), 0)

        @pl.when(inside)
        def _():
            sent(like_blocks(len(traced[1])), 1)


def fused(n_pipe, n_tensor, memory, states, norm_gain, w_query, w_keyvalue, w_output):
    seqs, pos, feat = memory.shape
    rows = states.shape[2]
    depth, inner = feat * n_tensor, w_query.shape[2]
    enc = pos * n_pipe
    xs, highs = n_tensor // CORES, n_pipe // LOW
    groups = 2 * inner // LANES
    weight_kv = w_keyvalue[0].reshape(depth, 2, inner // LANES, LANES)
    weight_kv = weight_kv.transpose(0, 2, 1, 3).reshape(depth * groups, LANES)
    blocks = n_pipe * xs
    tiles = feat // min(TILE, feat)
    copies = seqs * (xs + xs + 2 * xs + (xs - 1) * tiles) + 2
    any_space = pl.BlockSpec(memory_space=pl.ANY)
    in_vmem = pl.BlockSpec(memory_space=pltpu.VMEM)
    dma = pltpu.SemaphoreType.DMA
    out = pl.pallas_call(
        functools.partial(kernel, n_pipe, n_tensor),
        out_shape=jax.ShapeDtypeStruct((seqs, rows, feat), BF16),
        in_specs=[any_space, any_space, in_vmem, any_space, any_space, any_space],
        out_specs=any_space,
        scratch_shapes=[
            pltpu.VMEM((seqs, enc, depth), BF16),
            pltpu.VMEM((seqs, rows, depth), BF16),
            pltpu.VMEM((depth, inner), BF16),
            pltpu.VMEM((depth, 2 * inner), BF16),
            pltpu.VMEM((inner, depth), BF16),
            pltpu.VMEM((seqs, rows, max(inner, feat)), BF16),
            pltpu.VMEM((enc, 2 * inner), BF16),
            pltpu.VMEM((seqs, xs, rows, feat), BF16),
            pltpu.VMEM((seqs, xs, rows, feat), BF16),
            pltpu.VMEM((seqs, xs - 1, rows, feat), BF16),
            pltpu.VMEM((seqs, xs - 1, rows, feat), BF16),
            pltpu.VMEM((seqs, rows, feat), F32),
            pltpu.VMEM((SLOTS, CHUNK * groups, LANES), BF16),
            pltpu.VMEM((seqs, rows, LANES), F32),
            dma((6,)),
            dma((SLOTS,)),
            dma((copies,)),
            dma((seqs, blocks)),
            dma((seqs, LOW)),
            dma((seqs, xs)),
            dma((seqs, xs)),
            dma((seqs, xs, 2)),
            dma((seqs, xs - 1, tiles)),
            dma((seqs, tiles)),
        ],
        compiler_params=pltpu.CompilerParams(
            collective_id=0, has_side_effects=True, vmem_limit_bytes=67_000_000
        ),
    )(memory, states[0], norm_gain, w_query[0], weight_kv, w_output[0])
    return out[None]


def per_device(memory, states, norm_gain, w_query, w_keyvalue, w_output):
    whole_states = lax.all_gather(states[0], "tensor", axis=2, tiled=True)
    xf = whole_states.astype(jnp.float32)
    scale = lax.rsqrt(jnp.mean(xf * xf, axis=-1, keepdims=True) + 1e-06)
    normed = (xf * scale * norm_gain[0]).astype(jnp.bfloat16)
    weight_q = w_query[0]
    local_inner = weight_q.shape[1]
    weight_kv = w_keyvalue[0].reshape(w_keyvalue.shape[1], 2 * local_inner)
    weight_o = w_output[0]
    seqs = normed.shape[0]
    dec_rows = normed.shape[1]
    local_heads = local_inner // HEAD_DIM
    query = jnp.einsum("btd,de->bte", normed, weight_q, preferred_element_type=jnp.float32).astype(
        jnp.bfloat16
    )
    gathered = lax.all_gather(memory, "pipe", axis=1, tiled=True)
    gathered = lax.all_gather(gathered, "tensor", axis=2, tiled=True)
    keyvalue = jnp.einsum(
        "bpd,de->bpe", gathered, weight_kv, preferred_element_type=jnp.float32
    ).astype(jnp.bfloat16)
    enc_rows = keyvalue.shape[1]
    keys = keyvalue[:, :, :local_inner].reshape(seqs, enc_rows, local_heads, HEAD_DIM)
    values = keyvalue[:, :, local_inner:].reshape(seqs, enc_rows, local_heads, HEAD_DIM)
    heads_q = query.reshape(seqs, dec_rows, local_heads, HEAD_DIM)
    scores = jnp.einsum(
        "bqhd,bkhd->bhqk", heads_q, keys, preferred_element_type=jnp.float32
    ) / jnp.sqrt(jnp.float32(HEAD_DIM))
    probs = jax.nn.softmax(scores, axis=-1).astype(jnp.bfloat16)
    context = jnp.einsum(
        "bhqk,bkhd->bqhd", probs, values, preferred_element_type=jnp.float32
    ).astype(jnp.bfloat16)
    context = context.reshape(seqs, dec_rows, local_inner)
    partial_terms = jnp.einsum("bte,ed->btd", context, weight_o, preferred_element_type=jnp.float32)
    branch = lax.psum_scatter(partial_terms, "tensor", scatter_dimension=2, tiled=True)
    result = (states[0].astype(jnp.float32) + branch).astype(jnp.bfloat16)
    return result[None]


def solution(mesh):
    in_specs = (
        P(None, "pipe", "tensor"),
        P("pipe", None, None, "tensor"),
        P("pipe", None),
        P("pipe", None, "tensor"),
        P("pipe", None, None, "tensor"),
        P("pipe", "tensor", None),
    )
    out_specs = P("pipe", None, None, "tensor")
    n_pipe, n_tensor = mesh.shape["pipe"], mesh.shape["tensor"]
    even = n_pipe % LOW == 0 and n_tensor % CORES == 0 and n_pipe > LOW and n_tensor > CORES
    even = even and n_pipe // LOW == 4 and n_tensor // CORES == 2
    even = even and n_pipe // LOW == 4 and n_tensor // CORES == 2
    body = per_device
    if even and copies_per_sequence(n_pipe, n_tensor) <= MAX_COPIES:
        body = functools.partial(fused, n_pipe, n_tensor)
    return jax.shard_map(
        body, mesh=mesh, in_specs=in_specs, out_specs=out_specs, check_vma=False
    )
```

```python
import functools

import jax
import jax.numpy as jnp
from jax import lax
from jax.experimental import pallas as pl
from jax.experimental.pallas import tpu as pltpu
from jax.sharding import PartitionSpec as P

HEAD_DIM = 64
CORES = 2
LOW = 2
TILE = 256
WIDE = 512
MAX_COPIES = 100
LANES = 128
SUB = 16
CHUNK = 256
SLOTS = 3
PAIRS = 4
MESH = pl.DeviceIdType.MESH
F32 = jnp.float32
BF16 = jnp.bfloat16


def copies_per_sequence(n_pipe, n_tensor):
    xs, highs = n_tensor // CORES, n_pipe // LOW
    return 4 * n_pipe * xs + (xs - 1) * highs


def kernel(
    n_pipe, n_tensor,
    mem_hbm, st_hbm, gain_ref, wq_hbm, wkv_hbm, wo_hbm, out_hbm,
    mem, st, wq, wkv, wo, q, kv, pd, rd, px, rx, part, staged, squares,
    load_sem, stage_sem, send_sem, recv_ici, recv_d2d, st_ici, st_d2d, pd_sem, px_sem, out_sem,
):
    xs, highs = n_tensor // CORES, n_pipe // LOW
    seqs, enc, depth = mem.shape
    rows = st.shape[1]
    pos = enc // n_pipe
    feat = depth // n_tensor
    inner = wq.shape[1]
    pipe = lax.axis_index("pipe")
    tensor = lax.axis_index("tensor")
    hi, lo = pipe // LOW, pipe % LOW
    x, core = tensor // CORES, tensor % CORES
    other_lo, other_core = 1 - lo, 1 - core
    scope = jax.named_scope

    def turn(a, k, n):
        return lax.rem(a + k, n)

    def device(h, l, xx, c):
        return (h * LOW + l, xx * CORES + c)

    x_peers = [device(hi, lo, turn(x, j, xs), core) for j in range(1, xs)]
    pair = hi + 1 - 2 * lax.rem(hi, 2)
    inward = highs - 1 - hi
    inside = jnp.logical_and(hi > 0, hi < highs - 1)
    pair_peer = device(pair, lo, x, core)
    inward_peer = device(inward, lo, x, core)
    hi_sources = [pair, 2 - hi // 2, (highs - 1) * (1 - hi // 2)]
    lo_peer = device(hi, other_lo, x, core)
    sibling = device(hi, lo, x, other_core)

    def block(s, h, far, xx, c, at=None):
        at = hi if at is None else at
        near, away = lax.rem(h + at, 2), lax.rem(h // 2 + at // 2, 2)
        r = pl.multiple_of((away * highs + far * 2 + near) * pos, pos)
        f = pl.multiple_of((xx * CORES + c) * feat, feat)
        return mem.at[s, pl.ds(r, pos), pl.ds(f, feat)]

    def slot(h, l, xx):
        return (h * LOW + l) * xs + xx

    def st_block(s, xx, c):
        return st.at[s, :, pl.ds(pl.multiple_of((xx * CORES + c) * feat, feat), feat)]

    counter = [2]
    waits = []
    traced = [set(), set()]

    def remote(src, dst, sem, recv, dev):
        return pltpu.make_async_remote_copy(
            src_ref=src, dst_ref=dst, send_sem=send_sem.at[sem], recv_sem=recv,
            device_id=dev, device_id_type=MESH,
        )

    def send(src, dst, recv, dev, like, keep=True):
        sem = counter[0]
        counter[0] += 1
        remote(src, dst, sem, recv, dev).start()
        if keep:
            waits.append((like, sem))
        return sem

    def sent(like, sem):
        remote(like, like, sem, recv_ici.at[0, 0], sibling).wait_send()

    def like_block():
        return block(0, 0, 0, 0, 0)

    def like_blocks(n):
        return mem.at[:, :n * pos * feat // (seqs * depth), :]

    def send_block(src, dst, recv, dev, sem, *key):
        traced[sem].add(key)
        remote(src, dst, sem, recv, dev).start()

    def send_own(s, h, xx, dev, at, sem, *key):
        send_block(block(s, h, 0, xx, core), block(s, h, 0, xx, core, at),
                   recv_ici.at[s, slot(h, lo, xx)], dev, sem, "own", s, *key)

    def send_inward(s, h, xx, *key):
        @pl.when(inside)
        def _():
            send_own(s, h, xx, inward_peer, inward, 1, *key)

    def send_low(s, h, xx, *key):
        send_block(block(s, h, 0, xx, core), block(s, h, 1, xx, core),
                   recv_ici.at[s, slot(h, lo, xx)], lo_peer, 0, "low", s, *key)

    def send_over(s, h, far, away, xx, *key):
        ref = block(s, h, far, xx, core)
        send_block(ref, ref, recv_d2d.at[s, away], sibling, 0, "over", s, far, *key)

    def arrived(s, h, l, xx):
        ref = like_block()
        remote(ref, ref, 0, recv_ici.at[s, slot(h, l, xx)], sibling).wait_recv()

    st_sends = [[], []]

    def low_first(s):
        send_low(s, hi, x, "first")

    def across_first(s):
        for j, dev in enumerate(x_peers):
            send_own(s, hi, x, dev, hi, 0, "across", j)

    def high_first(s):
        send_own(s, hi, x, pair_peer, pair, 0, "first")
        send_inward(s, hi, x, "first")

    def over_first(s):
        send_over(s, hi, 0, 0, x, "first")

    def state_sends(s):
        ref = st_block(s, x, core)
        for dev in x_peers:
            st_sends[s].append(send(ref, ref, st_ici.at[s, x], dev, None, False))
        st_sends[s].append(send(ref, ref, st_d2d.at[s, x], sibling, None, False))

    def forward_x(s):
        for j in range(1, xs):
            xx = turn(x, j, xs)
            arrived(s, hi, lo, xx)
            send_own(s, hi, xx, pair_peer, pair, 0, j)
            send_inward(s, hi, xx, j)
            send_low(s, hi, xx, j)
            send_over(s, hi, 0, 0, xx, j)

    high_order = [(0, 0), (0, 1), (1, 0), (1, 1), (2, 0), (2, 1)]
    SIDEWAYS = (1, 3)
    low_order = [(None, j) for j in range(xs)] + high_order

    def forward_line(s, i):
        k, j = high_order[i]
        h, xx = hi_sources[k], turn(x, j, xs)
        arrived(s, h, lo, xx)
        send_own(s, h, xx, inward_peer if k == 0 else pair_peer, inward if k == 0 else pair, 1, "high", i)

    def forward_out(s, i):
        k, j = high_order[i]
        h, xx = hi_sources[k], turn(x, j, xs)
        if not (s == seqs - 1 and i in SIDEWAYS):
            send_low(s, h, xx, "high", i)
        send_over(s, h, 0, int(k > 0), xx, "high", i)

    def await_high(s, i):
        k, j = high_order[i]
        arrived(s, hi_sources[k], lo, turn(x, j, xs))

    def forward_low(s, i):
        k, j = low_order[i]
        h, xx = hi if k is None else hi_sources[k], turn(x, j, xs)
        arrived(s, h, other_lo, xx)
        if s == seqs - 1 and j == 0 and k in [high_order[i][0] for i in SIDEWAYS]:
            ref = block(s, h, 1, xx, core)
            send_block(ref, ref, recv_ici.at[s, slot(h, other_lo, xx)], x_peers[0], 0, "sideways", s, k)
        send_over(s, h, 1, int(k is not None and k > 0), xx, i)

    def forward_states(s):
        for j in range(1, xs):
            xx = turn(x, j, xs)
            ref = st_block(s, xx, core)
            remote(ref, ref, 0, st_ici.at[s, xx], sibling).wait_recv()
            st_sends[s].append(send(ref, ref, st_d2d.at[s, xx], sibling, None, False))

    def finish_states(s):
        for j in range(int(s == seqs - 1), xs):
            xx = turn(x, j, xs)
            ref = st_block(s, xx, other_core)
            remote(ref, ref, 0, st_d2d.at[s, xx], sibling).wait_recv()
        for sem in st_sends[s]:
            sent(st_block(s, x, core), sem)

    def finish_memory(s, away):
        ref = mem.at[s, :highs * pos, :xs * feat]
        remote(ref, ref, 0, recv_d2d.at[s, away], sibling).wait_recv()

    def steps(n, body, plan=()):
        plan = dict(plan)
        assert all(t < n for t in plan)

        @pl.loop(0, n)
        def _(i):
            for t, events in plan.items():
                @pl.when(i == t)
                def _(events=events):
                    do(*events)

            body(i)

    def do(*events):
        for fn, *args in events:
            if fn.__name__ in ("mid", "tip"):
                fn(*args)
            else:
                with scope("_".join([fn.__name__] + [str(a) for a in args])):
                    fn(*args)

    def set_scale(s):
        mean = jnp.sum(squares[s], axis=-1, keepdims=True) * (1.0 / depth)
        scale = lax.rsqrt(mean + 1e-06) * (HEAD_DIM ** -0.5)
        squares[s] = jnp.broadcast_to(scale, (rows, LANES))

    def normalize(s):
        part[s] = st[s, :, pl.ds(pl.multiple_of(tensor * feat, feat), feat)].astype(F32)

        @pl.loop(0, rows // SUB)
        def _(i):
            some = pl.ds(pl.multiple_of(i * SUB, SUB), SUB)
            total = jnp.zeros((SUB, LANES), F32)
            for g in range(depth // LANES):
                cols = slice(g * LANES, (g + 1) * LANES)
                xf = st[s, some, cols].astype(F32)
                total += xf * xf
                st[s, some, cols] = (xf * gain_ref[:, cols]).astype(BF16)
            squares[s, some, :] = total

        set_scale(s)

    def query(s, plan):
        def body(i):
            cols = pl.ds(pl.multiple_of(i * TILE, TILE), TILE)
            full = jnp.dot(st[s], wq[:, cols], preferred_element_type=F32)
            scale = squares[s]
            q[s, :, cols] = (full * jnp.concatenate([scale] * (TILE // LANES), axis=1)).astype(BF16)

        steps(inner // TILE, body, plan)

    def chip_features(xx, c):
        return pl.multiple_of((xx * CORES + c) * feat, feat)

    def early_query(s, plan):
        ref = st_block(s, x, other_core)
        remote(ref, ref, 0, st_d2d.at[s, x], sibling).wait_recv()

        @pl.loop(0, rows // SUB)
        def _(i):
            some = pl.ds(pl.multiple_of(i * SUB, SUB), SUB)
            total = jnp.zeros((SUB, LANES), F32)
            for c in range(CORES):
                for g in range(feat // LANES):
                    cols = pl.ds(pl.multiple_of(chip_features(x, c) + g * LANES, LANES), LANES)
                    xf = st[s, some, cols].astype(F32)
                    total += xf * xf
                    pd[s, c, some, g * LANES:(g + 1) * LANES] = (xf * gain_ref[:, cols]).astype(BF16)
            squares[s, some, :] = total

        def body(i):
            cols = pl.ds(pl.multiple_of(i * WIDE, WIDE), WIDE)
            part[s, :, cols] = sum(
                jnp.dot(pd[s, c], wq[pl.ds(chip_features(x, c), feat), cols], preferred_element_type=F32)
                for c in range(CORES)
            )

        steps(inner // WIDE, body, plan)

    def late_query(s, plan):
        xx = turn(x, 1, xs)

        @pl.loop(0, rows // SUB)
        def _(i):
            some = pl.ds(pl.multiple_of(i * SUB, SUB), SUB)
            total = squares[s, some, :]
            for c in range(CORES):
                for g in range(feat // LANES):
                    cols = pl.ds(pl.multiple_of(chip_features(xx, c) + g * LANES, LANES), LANES)
                    xf = st[s, some, cols].astype(F32)
                    total += xf * xf
                    st[s, some, cols] = (xf * gain_ref[:, cols]).astype(BF16)
            squares[s, some, :] = total

        set_scale(s)

        def body(i):
            cols = pl.ds(pl.multiple_of(i * WIDE, WIDE), WIDE)
            mine = pl.ds(chip_features(xx, 0), CORES * feat)
            full = part[s, :, cols] + jnp.dot(st[s, :, mine], wq[mine, cols], preferred_element_type=F32)
            q[s, :, cols] = (full * jnp.concatenate([squares[s]] * (WIDE // LANES), axis=1)).astype(BF16)

        steps(inner // WIDE, body, plan)
        part[s] = st[s, :, pl.ds(pl.multiple_of(tensor * feat, feat), feat)].astype(F32)

    half = highs * pos

    def keyvalue(s, far, plan, per=1):
        def body(i):
            for u in range(per):
                cols = pl.ds(pl.multiple_of((i * per + u) * WIDE, WIDE), WIDE)
                full = jnp.dot(mem[s, far * half:(far + 1) * half], wkv[:, cols], preferred_element_type=F32)
                kv[far * half:(far + 1) * half, cols] = full.astype(BF16)

        steps(2 * inner // (WIDE * per), body, plan)

    def attention(s, plan):
        lane = lax.broadcasted_iota(jnp.int32, (1, 2 * HEAD_DIM), 1)
        first = lane < HEAD_DIM

        def body(step):
            places = [pl.multiple_of((step * PAIRS + u) * 2 * HEAD_DIM, 2 * HEAD_DIM) for u in range(PAIRS)]
            scores, probs = [], []
            for c in places:
                qp, kp = q[s, :, pl.ds(c, 2 * HEAD_DIM)], kv[:, pl.ds(c, 2 * HEAD_DIM)]
                for mine in (first, jnp.logical_not(first)):
                    qh = jnp.where(mine, qp, jnp.zeros_like(qp))
                    scores.append(lax.dot_general(
                        qh, kp, (((1,), (1,)), ((), ())), preferred_element_type=F32
                    ))
            for one in scores:
                top = jnp.max(one, axis=-1, keepdims=True)
                probs.append(jnp.exp(one - top).astype(BF16))
            for u, c in enumerate(places):
                vp = kv[:, pl.ds(inner + c, 2 * HEAD_DIM)]
                both = jnp.concatenate([vp, jnp.ones_like(vp)], axis=1)
                outs = [jnp.dot(probs[2 * u + e], both, preferred_element_type=F32) for e in range(2)]
                total = jnp.where(first, outs[0][:, :2 * HEAD_DIM], outs[1][:, :2 * HEAD_DIM])
                sums = jnp.where(first, outs[0][:, 2 * HEAD_DIM:], outs[1][:, 2 * HEAD_DIM:])
                q[s, :, pl.ds(c, 2 * HEAD_DIM)] = (total / sums).astype(BF16)

        steps(inner // (2 * HEAD_DIM * PAIRS), body, plan)

    cuts = [slice(i, i + min(WIDE, feat)) for i in range(0, feat, min(WIDE, feat))]

    pieces = [slice(i, i + min(TILE, feat)) for i in range(0, feat, min(TILE, feat))]

    def product(s, t, c):
        cols = pl.ds(pl.multiple_of(t * feat + c.start, LANES), c.stop - c.start)
        return jnp.dot(q[s, :, :inner], wo[:, cols], preferred_element_type=F32)

    order = [turn(x, j, xs) for j in range(1, xs)] + [x]
    last = xs - 1
    whole = slice(0, feat)
    lead, rest = [pieces[0]], [slice(pieces[1].start, cuts[0].stop)] + cuts[1:]

    def bounds(group):
        return slice(group[0].start, group[-1].stop)

    def over(s, j, group):
        for c in group:
            pd[s, j, :, c] = product(s, order[j] * CORES + other_core, c).astype(BF16)

    def mine(s, j, group):
        for c in group:
            px[s, j, :, c] = product(s, order[j] * CORES + core, c).astype(BF16)

    def over_send(s, j, g, c):
        send(pd.at[s, j, :, c], rd.at[s, j, :, c], pd_sem.at[s, j, g], sibling, lambda: pd.at[0, 0, :, c])

    def back(s, j, g, c):
        remote(pd.at[s, j, :, c], rd.at[s, j, :, c], 0, pd_sem.at[s, j, g], sibling).wait_recv()

    def pass_on(s, g, b):
        for j in range(last):
            back(s, j, g, b)
            for i, c in enumerate(pieces):
                if b.start <= c.start < b.stop:
                    px[s, j, :, c] = (px[s, j, :, c].astype(F32) + rd[s, j, :, c].astype(F32)).astype(BF16)
                    send(px.at[s, j, :, c], rx.at[s, j, :, c], px_sem.at[s, j, i], x_peers[j],
                         lambda c=c: pd.at[0, 0, :, c])

    def output(s):
        for j in range(last):
            over(s, j, cuts)
            mine(s, j, cuts)
            over_send(s, j, 0, whole)

    def output_early(s):
        for j in range(last):
            over(s, j, lead)
            over_send(s, j, 0, bounds(lead))
            mine(s, j, lead)
            over(s, j, rest)
            over_send(s, j, 1, bounds(rest))
        pass_on(s, 0, bounds(lead))
        for j in range(last):
            mine(s, j, rest)
        pass_on(s, 1, bounds(rest))

    def output_here(s):
        over(s, last, cuts)
        over_send(s, last, 0, whole)
        for c in cuts:
            part[s, :, c] += product(s, tensor, c)

    def out_copy(s, i, c):
        return pltpu.make_async_copy(q.at[s, :, c], out_hbm.at[s, :, c], out_sem.at[s, i])

    def finish(s):
        back(s, last, 0, whole)
        for i, c in enumerate(pieces):
            part[s, :, c] += rd[s, last, :, c].astype(F32)
        for i, c in enumerate(pieces):
            total = part[s, :, c]
            for j in range(xs - 1):
                remote(px.at[s, j, :, c], rx.at[s, j, :, c], 0, px_sem.at[s, j, i], sibling).wait_recv()
                total += rx[s, j, :, c].astype(F32)
            q[s, :, c] = total.astype(BF16)
            out_copy(s, i, c).start()

    groups = 2 * inner // LANES
    size = CHUNK * groups
    chunks = depth // CHUNK
    slots = staged.shape[0]

    def stage(i, slot):
        src = wkv_hbm.at[pl.ds(pl.multiple_of(i * size, size), size), :]
        return pltpu.make_async_copy(src, staged.at[slot], stage_sem.at[slot])

    def spread(plan):
        span = SUB * groups
        a = lax.broadcasted_iota(jnp.int32, (span, span), 0)
        b = lax.broadcasted_iota(jnp.int32, (span, span), 1)
        swap = (b == lax.rem(a, SUB) * groups + a // SUB).astype(F32).astype(BF16)

        def body(i):
            slot = lax.rem(i, slots)
            stage(i, slot).wait()
            for m in range(CHUNK // (2 * SUB)):
                r = m * 2 * span
                both = jnp.concatenate(
                    [staged[slot, r:r + span, :], staged[slot, r + span:r + 2 * span, :]], axis=1
                )
                moved = jnp.dot(swap, both, preferred_element_type=F32).astype(BF16)
                d = pl.multiple_of(i * CHUNK + m * 2 * SUB, 2 * SUB)
                for g in range(groups):
                    col = (g % 2) * inner + (g // 2) * LANES
                    piece = moved[g * SUB:(g + 1) * SUB]
                    wkv[pl.ds(d, SUB), col:col + LANES] = piece[:, :LANES]
                    wkv[pl.ds(d + SUB, SUB), col:col + LANES] = piece[:, LANES:]

            @pl.when(i + slots < chunks)
            def _():
                stage(i + slots, slot).start()

        steps(chunks, body, plan)

    loads = [
        pltpu.make_async_copy(mem_hbm.at[0], block(0, hi, 0, x, core), load_sem.at[0]),
        pltpu.make_async_copy(st_hbm.at[0], st_block(0, x, core), load_sem.at[1]),
        pltpu.make_async_copy(mem_hbm.at[1], block(1, hi, 0, x, core), load_sem.at[2]),
        pltpu.make_async_copy(st_hbm.at[1], st_block(1, x, core), load_sem.at[3]),
    ]
    weights = [
        pltpu.make_async_copy(wq_hbm, wq, load_sem.at[4]),
        pltpu.make_async_copy(wo_hbm, wo, load_sem.at[5]),
    ]
    for copy in loads:
        copy.start()
    barrier = pltpu.get_barrier_semaphore()
    peers = x_peers + [pair_peer, lo_peer, sibling]
    for peer in peers:
        pl.semaphore_signal(barrier, inc=1, device_id=peer, device_id_type=MESH)

    @pl.when(inside)
    def _():
        pl.semaphore_signal(barrier, inc=1, device_id=inward_peer, device_id_type=MESH)

    for i in range(slots):
        stage(i, i).start()
    with scope("barrier"):
        pl.semaphore_wait(barrier, len(peers) + lax.rem(hi + hi // 2, 2))
    with scope("load0"):
        loads[0].wait()
    across_first(0)
    low_first(0)
    high_first(0)
    over_first(0)
    with scope("load1"):
        loads[1].wait()
    state_sends(0)
    loads[2].wait()
    low_first(1)
    high_first(1)
    across_first(1)
    over_first(1)
    loads[3].wait()
    state_sends(1)

    outside = jnp.logical_not(inside)

    def load(i): weights[i].start()

    def across(s): pass_on(s, 0, whole)

    def fx(s): forward_x(s)

    def fl(s, i): forward_low(s, i)

    def mid(*events):
        @pl.when(inside)
        def _():
            do(*events)

    def tip(*events):
        @pl.when(outside)
        def _():
            do(*events)

    def ml(s, i): forward_line(s, i)

    def fo(s, i): forward_out(s, i)

    def fi(s, i):
        forward_line(s, i)
        forward_out(s, i)

    def ft(s, i):
        await_high(s, i)
        forward_out(s, i)

    with scope("spread"):
        spread({
            6: [(fx, 0), (fl, 0, 0), (mid, (fi, 0, 0), (ml, 0, 2)), (tip, (ft, 0, 0))],
            10: [(load, 0)],
            12: [(fl, 0, 1), (mid, (fi, 0, 1), (fo, 0, 2), (fi, 0, 3)), (tip, (ft, 0, 1))],
        })
    do((load, 1), (mid, (fi, 0, 4)), (tip, (ft, 0, 2)), (fl, 0, 2))
    weights[0].wait()
    with scope("early"):
        early_query(1, {1: [(mid, (fi, 0, 5))]})
    do((fl, 0, 3), (tip, (ft, 0, 3)))
    with scope("finmem00"):
        finish_memory(0, 0)
    with scope("kv00"):
        keyvalue(0, 0, {
            0: [(forward_states, 0)],
            1: [(tip, (ft, 0, 4)), (fl, 0, 4)],
        }, 2)
    do((tip, (ft, 0, 5)), (fx, 1), (fl, 0, 5))
    with scope("finst0"):
        finish_states(0)
    with scope("norm0"):
        normalize(0)
    with scope("query0"):
        query(0, {
            1: [(fl, 0, 6)],
            2: [(mid, (fi, 1, 0), (ml, 1, 2)), (tip, (ft, 1, 0))],
        })
    do((mid, (fi, 1, 1), (fo, 1, 2), (fi, 1, 3)), (tip, (ft, 1, 1)), (fl, 0, 7))
    with scope("finmem01"):
        finish_memory(0, 1)
    with scope("kv01"):
        keyvalue(0, 1, {
            1: [(fl, 1, 0), (tip, (ft, 1, 2)), (mid, (fi, 1, 4))],
        }, 2)
    do((forward_states, 1), (fl, 1, 1))
    with scope("att0"):
        attention(0, {
            0: [(mid, (fi, 1, 5)), (tip, (ft, 1, 3)), (fl, 1, 2)],
        })
    with scope("finst1"):
        finish_states(1)
    with scope("query1"):
        late_query(1, {
            0: [(tip, (ft, 1, 4))],
            1: [(tip, (ft, 1, 5)), (fl, 1, 4), (fl, 1, 3)],
        })
    weights[1].wait()
    with scope("output0"):
        output(0)
    with scope("finmem10"):
        finish_memory(1, 0)
    with scope("kv10"):
        keyvalue(1, 0, {1: [(across, 0), (fl, 1, 6)]}, 2)
    do((fl, 1, 5), (fl, 1, 7))
    with scope("finmem11"):
        finish_memory(1, 1)
    with scope("kv11"):
        keyvalue(1, 1, {}, 2)
    with scope("att1"):
        attention(1, {})
    with scope("output1"):
        output_early(1)
    with scope("here0"):
        output_here(0)
    with scope("here1"):
        output_here(1)
    with scope("finish0"):
        finish(0)
    with scope("finish1"):
        finish(1)
    assert [len(t) for t in traced] == [54, 16], [len(t) for t in traced]
    with scope("end"):
        for like, sem in waits:
            sent(like(), sem)
        for s in range(seqs):
            for i, c in enumerate(pieces):
                out_copy(s, i, c).wait()
        sent(like_blocks(len(traced[0])), 0)

        @pl.when(inside)
        def _():
            sent(like_blocks(len(traced[1])), 1)


def fused(n_pipe, n_tensor, memory, states, norm_gain, w_query, w_keyvalue, w_output):
    seqs, pos, feat = memory.shape
    rows = states.shape[2]
    depth, inner = feat * n_tensor, w_query.shape[2]
    enc = pos * n_pipe
    xs, highs = n_tensor // CORES, n_pipe // LOW
    groups = 2 * inner // LANES
    weight_kv = w_keyvalue[0].reshape(depth, 2, inner // LANES, LANES)
    weight_kv = weight_kv.transpose(0, 2, 1, 3).reshape(depth * groups, LANES)
    blocks = n_pipe * xs
    tiles = feat // min(TILE, feat)
    copies = seqs * (xs + xs + 2 * xs + (xs - 1) * tiles) + 2
    any_space = pl.BlockSpec(memory_space=pl.ANY)
    in_vmem = pl.BlockSpec(memory_space=pltpu.VMEM)
    dma = pltpu.SemaphoreType.DMA
    out = pl.pallas_call(
        functools.partial(kernel, n_pipe, n_tensor),
        out_shape=jax.ShapeDtypeStruct((seqs, rows, feat), BF16),
        in_specs=[any_space, any_space, in_vmem, any_space, any_space, any_space],
        out_specs=any_space,
        scratch_shapes=[
            pltpu.VMEM((seqs, enc, depth), BF16),
            pltpu.VMEM((seqs, rows, depth), BF16),
            pltpu.VMEM((depth, inner), BF16),
            pltpu.VMEM((depth, 2 * inner), BF16),
            pltpu.VMEM((inner, depth), BF16),
            pltpu.VMEM((seqs, rows, max(inner, feat)), BF16),
            pltpu.VMEM((enc, 2 * inner), BF16),
            pltpu.VMEM((seqs, xs, rows, feat), BF16),
            pltpu.VMEM((seqs, xs, rows, feat), BF16),
            pltpu.VMEM((seqs, xs - 1, rows, feat), BF16),
            pltpu.VMEM((seqs, xs - 1, rows, feat), BF16),
            pltpu.VMEM((seqs, rows, feat), F32),
            pltpu.VMEM((SLOTS, CHUNK * groups, LANES), BF16),
            pltpu.VMEM((seqs, rows, LANES), F32),
            dma((6,)),
            dma((SLOTS,)),
            dma((copies,)),
            dma((seqs, blocks)),
            dma((seqs, LOW)),
            dma((seqs, xs)),
            dma((seqs, xs)),
            dma((seqs, xs, 2)),
            dma((seqs, xs - 1, tiles)),
            dma((seqs, tiles)),
        ],
        compiler_params=pltpu.CompilerParams(
            collective_id=0, has_side_effects=True, vmem_limit_bytes=67_000_000
        ),
    )(memory, states[0], norm_gain, w_query[0], weight_kv, w_output[0])
    return out[None]


def per_device(memory, states, norm_gain, w_query, w_keyvalue, w_output):
    whole_states = lax.all_gather(states[0], "tensor", axis=2, tiled=True)
    xf = whole_states.astype(jnp.float32)
    scale = lax.rsqrt(jnp.mean(xf * xf, axis=-1, keepdims=True) + 1e-06)
    normed = (xf * scale * norm_gain[0]).astype(jnp.bfloat16)
    weight_q = w_query[0]
    local_inner = weight_q.shape[1]
    weight_kv = w_keyvalue[0].reshape(w_keyvalue.shape[1], 2 * local_inner)
    weight_o = w_output[0]
    seqs = normed.shape[0]
    dec_rows = normed.shape[1]
    local_heads = local_inner // HEAD_DIM
    query = jnp.einsum("btd,de->bte", normed, weight_q, preferred_element_type=jnp.float32).astype(
        jnp.bfloat16
    )
    gathered = lax.all_gather(memory, "pipe", axis=1, tiled=True)
    gathered = lax.all_gather(gathered, "tensor", axis=2, tiled=True)
    keyvalue = jnp.einsum(
        "bpd,de->bpe", gathered, weight_kv, preferred_element_type=jnp.float32
    ).astype(jnp.bfloat16)
    enc_rows = keyvalue.shape[1]
    keys = keyvalue[:, :, :local_inner].reshape(seqs, enc_rows, local_heads, HEAD_DIM)
    values = keyvalue[:, :, local_inner:].reshape(seqs, enc_rows, local_heads, HEAD_DIM)
    heads_q = query.reshape(seqs, dec_rows, local_heads, HEAD_DIM)
    scores = jnp.einsum(
        "bqhd,bkhd->bhqk", heads_q, keys, preferred_element_type=jnp.float32
    ) / jnp.sqrt(jnp.float32(HEAD_DIM))
    probs = jax.nn.softmax(scores, axis=-1).astype(jnp.bfloat16)
    context = jnp.einsum(
        "bhqk,bkhd->bqhd", probs, values, preferred_element_type=jnp.float32
    ).astype(jnp.bfloat16)
    context = context.reshape(seqs, dec_rows, local_inner)
    partial_terms = jnp.einsum("bte,ed->btd", context, weight_o, preferred_element_type=jnp.float32)
    branch = lax.psum_scatter(partial_terms, "tensor", scatter_dimension=2, tiled=True)
    result = (states[0].astype(jnp.float32) + branch).astype(jnp.bfloat16)
    return result[None]


def solution(mesh):
    in_specs = (
        P(None, "pipe", "tensor"),
        P("pipe", None, None, "tensor"),
        P("pipe", None),
        P("pipe", None, "tensor"),
        P("pipe", None, None, "tensor"),
        P("pipe", "tensor", None),
    )
    out_specs = P("pipe", None, None, "tensor")
    n_pipe, n_tensor = mesh.shape["pipe"], mesh.shape["tensor"]
    even = n_pipe % LOW == 0 and n_tensor % CORES == 0 and n_pipe > LOW and n_tensor > CORES
    even = even and n_pipe // LOW == 4 and n_tensor // CORES == 2
    even = even and n_pipe // LOW == 4 and n_tensor // CORES == 2
    body = per_device
    if even and copies_per_sequence(n_pipe, n_tensor) <= MAX_COPIES:
        body = functools.partial(fused, n_pipe, n_tensor)
    return jax.shard_map(
        body, mesh=mesh, in_specs=in_specs, out_specs=out_specs, check_vma=False
    )
```
